256 devices in a mesh: section: 2 (over core), dp: 16 (over z, x_lo), tensor: 8 (over y, x_hi).
Axes of the slice: x: 4 (x_hi: 2, x_lo: 2; x = x_hi * 2 + x_lo), y: 4, z: 8, core: 2. Of those that a mesh axis runs over, the one named last changes fastest.
Arguments:
- tokens: bfloat16 [2048, 4096], P('dp', 'tensor'), may hold values from -6 to 6
- gain: bfloat16 [2, 4096], P('section', 'tensor'), may hold values from 0.099609375 to 1.8984375
- w_up: bfloat16 [2, 4096, 5120], P('section', 'dp', 'tensor'), may hold values from -0.09375 to 0.09375
- w_down: bfloat16 [2, 5120, 4096], P('section', 'tensor', 'dp'), may hold values from -0.078125 to 0.078125
- cotangent: bfloat16 [2, 2048, 4096], P('section', 'dp'), may hold values from -6 to 6
Outputs:
- states: bfloat16 [2, 2048, 4096], P('section', 'dp', 'tensor')
- grad_down: bfloat16 [2, 5120, 4096], P('section', 'tensor', 'dp')
The draws below stay inside these ranges and needn't reach their ends.
All inputs are finite; a program needn't handle non-finite values.
Results may differ from the reference program's by a relative error of at most 0.02.
Values may be sent and summed in bfloat16 or wider, within the bound.
A program may use at most 64 MiB of HBM per device.

```python
import jax
import jax.numpy as jnp
from jax import lax

WIDTH = 4096
HIDDEN_SIZE = 5120
TOK_DEV = 128
TOKENS = 2048
LAYERS = 2
N_SECTION = 2
N_DP = 16
N_TENSOR = 8


def block_levels(own_key, dims, pieces, low, high):
    level = 1.0
    for dim, blocks in pieces:
        steps = jax.random.uniform(jax.random.fold_in(jax.random.fold_in(own_key, 6), dim), (blocks,), jnp.float32, low / len(pieces), high / len(pieces))
        level = level * jnp.repeat(jnp.exp(steps), dims[dim] // blocks).reshape((-1,) + (1,) * (len(dims) - 1 - dim))
    return level


def normal_values(key, extent, deviation, bound, cuts=(), dtype=jnp.bfloat16):
    drawn = deviation * jax.random.normal(key, extent, jnp.float32)
    if cuts:
        drawn = drawn * block_levels(key, extent, cuts, -0.22, 0.18)
    return jnp.clip(drawn, -bound, bound).astype(dtype)


def setup_inputs(seed: int = 0) -> dict:
    arg_keys = jax.random.split(jax.random.key(seed), 6)
    return {
        "tokens": normal_values(arg_keys[0], (TOKENS, WIDTH), 1.0, 6.0, ((0, 16), (1, 8))),
        "gain": jnp.clip(1.0 + 0.18 * jax.random.normal(arg_keys[1], (LAYERS, WIDTH), jnp.float32), 0.099609375, 1.8984375).astype(jnp.bfloat16),
        "w_up": normal_values(arg_keys[2], (LAYERS, WIDTH, HIDDEN_SIZE), WIDTH ** -0.5, 0.09375, ((0, 2), (1, 16), (2, 8))),
        "w_down": normal_values(arg_keys[3], (LAYERS, HIDDEN_SIZE, WIDTH), HIDDEN_SIZE ** -0.5, 0.078125, ((0, 2), (1, 8), (2, 16))),
        "cotangent": normal_values(arg_keys[4], (LAYERS, TOKENS, WIDTH), 1.0, 6.0, ((0, 2), (1, 16))),
    }


EPS = 1e-06

def layer_ref(acts, gain_row, up_mat, down_mat):
    acts_f = acts.astype(jnp.float32)
    mean_sq = lax.optimization_barrier(jnp.mean(acts_f * acts_f, axis=1, keepdims=True))
    normed = (acts_f * lax.rsqrt(mean_sq + EPS) * gain_row.astype(jnp.float32)).astype(jnp.bfloat16)
    pre_act = jnp.dot(normed, up_mat, preferred_element_type=jnp.float32)
    hidden = jax.nn.gelu(pre_act, approximate=True).astype(jnp.bfloat16)
    group_width = HIDDEN_SIZE // N_TENSOR
    summed = jnp.zeros(acts.shape, jnp.float32)
    for group_id in range(N_TENSOR):
        lower = group_id * group_width
        partial_value = jnp.dot(hidden[:, lower:lower + group_width], down_mat[lower:lower + group_width, :], preferred_element_type=jnp.float32).astype(jnp.bfloat16)
        summed = summed + lax.optimization_barrier(partial_value).astype(jnp.float32)
    return ((acts_f + summed).astype(jnp.bfloat16), hidden)

def reference(tokens, gain, w_up, w_down, cotangent):
    acts = tokens
    states = []
    grads = []
    for layer_id in range(N_SECTION):
        acts, hidden = layer_ref(acts, gain[layer_id], w_up[layer_id], w_down[layer_id])
        states.append(acts)
        grad_sum = jnp.zeros((HIDDEN_SIZE, WIDTH), jnp.float32)
        for peer_id in range(N_DP):
            lower = peer_id * TOK_DEV
            partial_value = lax.dot_general(hidden[lower:lower + TOK_DEV], cotangent[layer_id][lower:lower + TOK_DEV], (((0,), (0,)), ((), ())), preferred_element_type=jnp.float32).astype(jnp.bfloat16)
            grad_sum = grad_sum + lax.optimization_barrier(partial_value).astype(jnp.float32)
        grads.append(grad_sum.astype(jnp.bfloat16))
    return (jnp.stack(states), jnp.stack(grads))
```

```python
import functools

import jax
import jax.numpy as jnp
from jax import lax
from jax.experimental import pallas as pl
from jax.experimental.pallas import tpu as pltpu
from jax.sharding import PartitionSpec as P

EPS = 1e-06
F32 = jnp.float32
BF16 = jnp.bfloat16

MESH = pl.DeviceIdType.MESH
LANES = 128
PIECES = 2
INNER = 2


def far_first(count):
    return sorted(range(1, count), key=lambda k: abs(2 * k - count))


def remote(src, dst, send_sem, recv_sem, target):
    return pltpu.make_async_remote_copy(
        src_ref=src,
        dst_ref=dst,
        send_sem=send_sem,
        recv_sem=recv_sem,
        device_id=target,
        device_id_type=MESH,
    )


def stack_kernel(
    sizes,
    width,
    tok_ref,
    gain_ref,
    up_ref,
    down_ref,
    cot_ref,
    state_out,
    grad_out,
    tok,
    gain_f,
    gains,
    wu,
    wd,
    xb,
    xg,
    ssq,
    acc,
    sq_send,
    sq_recv,
    up_send,
    up_recv,
    hid,
    part_send,
    part_recv,
    state_buf,
    hg,
    cb,
    gacc,
    gsend,
    grecv,
    ld,
    tk_ss,
    tk_rs,
    ga_ss,
    ga_rs,
    z_ss,
    z_rs,
    f_ss,
    f_rs,
    c_ss,
    c_rs,
    cs_ss,
    cs_rs,
    sq_ss,
    sq_rs,
    ux_ss,
    ux_rs,
    ax_ss,
    ax_rs,
    hd_ss,
    hd_rs,
    h_ss,
    h_rs,
    p_ss,
    p_rs,
    x_ss,
    x_rs,
    st_ss,
    st_rs,
    gx_ss,
    gx_rs,
    end_sem,
):
    sections, dp_count, nt = sizes
    nz = dp_count // INNER
    hi = nz // 2
    lo = nz - 1 - hi
    rows, slice_width = tok.shape
    h2 = rows // sections
    feat = slice_width // INNER
    part_rows = rows // nt
    hidden = wu.shape[3]

    core = lax.axis_index("section")
    t = lax.axis_index("tensor")
    me = lax.axis_index("dp")
    z = me // INNER
    q = lax.rem(me, INNER)
    other = 1 - core
    sign = 1 - 2 * core
    beside = z * INNER + 1 - q

    def block_of(index, size):
        return pl.ds(pl.multiple_of(index * size, size), size)

    mine = block_of(q, h2)
    theirs = block_of(1 - q, h2)
    core_rows = block_of(core, h2)
    other_rows = block_of(other, h2)
    my_cols = block_of(q, feat)
    their_cols = block_of(1 - q, feat)
    my_part = block_of(t, part_rows)

    def tensor_at(off):
        return lax.rem(t + off, nt)

    def plane_at(shift):
        return lax.rem(z + nz + shift, nz)

    sends = []

    def launch(make, *args, cond=None):
        make = functools.partial(make, *args)
        sends.append((make, cond))
        if cond is None:
            make().start()
        else:
            pl.when(cond())(lambda: make().start())

    loads = [
        pltpu.make_async_copy(up_ref.at[0], wu.at[core, z], ld.at[0]),
        pltpu.make_async_copy(tok_ref, tok, ld.at[1]),
        pltpu.make_async_copy(down_ref.at[0], wd.at[core, z], ld.at[2]),
        pltpu.make_async_copy(
            cot_ref.at[0, my_part, block_of(z, slice_width)], cb.at[z, my_part], ld.at[3]
        ),
    ]
    for copy in loads:
        copy.start()

    barrier = pltpu.get_barrier_semaphore()

    def greet(target):
        pl.semaphore_signal(barrier, inc=1, device_id=target, device_id_type=MESH)

    for m in far_first(nz):
        greet({"dp": plane_at(m) * INNER + q})
    for off in far_first(nt) + [0]:
        greet({"dp": beside, "tensor": tensor_at(off)})
        greet({"section": other, "tensor": tensor_at(off)})
        if off:
            greet({"tensor": tensor_at(off)})
    greet({"section": other, "dp": beside})

    gain_f[...] = gain_ref[...].astype(F32)
    gains[core, t] = gain_f[:, my_cols]
    ssq[...] = jnp.zeros_like(ssq)
    for copy in loads:
        copy.wait()
    xb[0, t, mine] = tok[core_rows, my_cols]

    pl.semaphore_wait(barrier, (nz - 1) + (2 * nt - 1) + nt + 1)

    def weight(layer, kind, origin, piece):
        buf = wd if kind else wu
        size = buf.shape[2] // PIECES
        return buf.at[layer, origin, pl.ds(piece * size, size)]

    def along(d):
        return plane_at(-sign * d)

    def against(d):
        return plane_at(sign * d)

    def hop(m, piece, s):
        ref = weight(m // 2, m % 2, along(s), piece)
        return remote(
            ref,
            ref,
            z_ss.at[m, piece, s],
            z_rs.at[m, piece, s],
            {"dp": plane_at(sign) * INNER + q},
        )

    def landing(m, piece, d):
        ref = weight(m // 2, m % 2, along(d), piece)
        return remote(
            ref,
            ref,
            z_ss.at[m, piece, d - 1],
            z_rs.at[m, piece, d - 1],
            {"dp": plane_at(sign) * INNER + q},
        )

    def push(m, piece, d):
        ref = weight(m // 2, m % 2, along(d), piece)
        return remote(
            ref, ref, f_ss.at[m, piece, d], f_rs.at[m, piece, d], {"section": other}
        )

    def pushed(m, piece, d):
        ref = weight(m // 2, m % 2, against(d), piece)
        return remote(
            ref, ref, f_ss.at[m, piece, d], f_rs.at[m, piece, d], {"section": other}
        )

    def push_own(kind, piece):
        ref = weight(core, kind, z, piece)
        m = 2 * core + kind
        return remote(
            ref, ref, f_ss.at[m, piece, 0], f_rs.at[m, piece, 0], {"section": other}
        )

    def holds(layer):
        return lambda: core == layer

    def lacks(layer):
        return lambda: core != layer

    def pass_on(m, piece, s):
        if s < lo:
            launch(hop, m, piece, s)
        elif s < hi:
            launch(hop, m, piece, s, cond=holds(m // 2))

    def advance(m, d):
        layer = m // 2
        for piece in range(PIECES):
            if d == 0:

                @pl.when(core != layer)
                def _():
                    pushed(m, piece, 0).wait_recv()

                pass_on(m, piece, 0)
            elif d <= lo:
                landing(m, piece, d).wait_recv()
                pass_on(m, piece, d)
                launch(push, m, piece, d)
            else:

                @pl.when(core == layer)
                def _():
                    landing(m, piece, d).wait_recv()

                launch(push, m, piece, d, cond=holds(layer))

    def take(m, d):
        for piece in range(PIECES):
            pushed(m, piece, d).wait_recv()

    def take_far(m):
        @pl.when(core != m // 2)
        def _():
            take(m, hi)

    for piece in range(PIECES):
        launch(push_own, 0, piece)

    @pl.when(core == 0)
    def _():
        for piece in range(PIECES):
            hop(0, piece, 0).start()

    def token_copy(away, off):
        cols, dp = (their_cols, beside) if away else (my_cols, me)
        return remote(
            tok.at[core_rows, cols],
            xb.at[0, t, mine],
            tk_ss.at[away, off],
            tk_rs.at[t, q],
            {"dp": dp, "tensor": tensor_at(off)},
        )

    def token_landing(tensor, cls):
        ref = xb.at[0, tensor, block_of(cls, h2)]
        return remote(ref, ref, tk_ss.at[0, 0], tk_rs.at[tensor, cls], {"dp": beside})

    for off in far_first(nt) + [0]:
        launch(token_copy, 1, off)
        if off:
            launch(token_copy, 0, off)

    def gain_copy(away, off):
        return remote(
            gains.at[core, t],
            gains.at[core, t],
            ga_ss.at[away, off],
            ga_rs.at[core, t],
            {"section": other if away else core, "tensor": tensor_at(off)},
        )

    def gain_landing(layer, tensor):
        ref = gains.at[layer, tensor]
        return remote(ref, ref, ga_ss.at[0, 0], ga_rs.at[layer, tensor], {"section": other})

    for off in far_first(nt) + [0]:
        launch(gain_copy, 1, off)
        if off:
            launch(gain_copy, 0, off)
    for piece in range(PIECES):
        launch(push_own, 1, piece)

    def cot_copy(m):
        to = plane_at(m)
        return remote(
            cot_ref.at[0, my_part, block_of(to, slice_width)],
            cb.at[z, my_part],
            c_ss.at[m],
            c_rs.at[z],
            {"dp": to * INNER + q},
        )

    def cot_landing(origin):
        ref = cb.at[origin, my_part]
        return remote(ref, ref, c_ss.at[0], c_rs.at[origin], {"dp": beside})

    @pl.when(core != 0)
    def _():
        for piece in range(PIECES):
            pushed(0, piece, 0).wait_recv()
            if lo:
                hop(0, piece, 0).start()

    for piece in range(PIECES):
        sends.append((functools.partial(hop, 0, piece, 0), None if lo else holds(0)))
    for m in far_first(nz):
        launch(cot_copy, m)

    def cot_share(off):
        ref = cb.at[:, my_part]
        return remote(ref, ref, cs_ss.at[off], cs_rs.at[t], {"tensor": tensor_at(off)})

    def cot_share_landing(tensor):
        ref = cb.at[:, block_of(tensor, part_rows)]
        return remote(ref, ref, cs_ss.at[0], cs_rs.at[tensor], {"dp": beside})

    def share_cotangent():
        for m in range(1, nz):
            cot_landing(plane_at(m)).wait_recv()
        for off in far_first(nt):
            launch(cot_share, off)

    def prepare(layer, block):
        x = xb[layer, block].astype(F32)
        xg[block] = (x * gains[layer, block]).astype(BF16)
        square = x * x
        total = ssq[...]
        for lower in range(0, feat, LANES):
            total = total + square[:, lower : lower + LANES]
        ssq[...] = total

    def up_block(layer, block, first=False):
        value = jnp.dot(xg[block], wu[layer, block], preferred_element_type=F32)
        acc[...] = value if first else acc[...] + value

    def sum_copy(layer):
        return remote(
            sq_send.at[layer], sq_recv.at[layer], sq_ss.at[layer], sq_rs.at[layer], {"dp": beside}
        )

    def send_sums(layer):
        sq_send[layer] = jnp.broadcast_to(
            jnp.sum(ssq[theirs], axis=1, keepdims=True), (h2, LANES)
        )
        launch(sum_copy, layer)

    def up_copy(layer):
        return remote(
            up_send.at[layer], up_recv.at[layer], ux_ss.at[layer], ux_rs.at[layer], {"dp": beside}
        )

    def send_up(layer):
        up_send[layer] = acc[theirs].astype(BF16)
        launch(up_copy, layer)

    def hidden_copy(layer):
        ref = hid.at[layer, mine]
        return remote(ref, ref, ax_ss.at[layer], ax_rs.at[layer], {"dp": beside})

    def hidden_landing(layer):
        ref = hid.at[layer, theirs]
        return remote(ref, ref, ax_ss.at[layer], ax_rs.at[layer], {"dp": beside})

    def hidden_give(layer):
        return remote(
            hid.at[layer, mine],
            hg.at[z, core_rows],
            hd_ss.at[layer],
            hd_rs.at[layer],
            {"section": other},
        )

    def hidden_given(layer):
        ref = hg.at[z, other_rows]
        return remote(ref, ref, hd_ss.at[layer], hd_rs.at[layer], {"section": other})

    def finish_up(layer):
        sum_copy(layer).wait_recv()
        total = jnp.sum(ssq[mine], axis=1, keepdims=True) + sq_recv[layer]
        inverse = lax.rsqrt(total / width + EPS)
        up_copy(layer).wait_recv()
        for lower in range(0, hidden, LANES):
            cols = pl.ds(lower, LANES)
            value = (acc[mine, cols] + up_recv[layer, :, cols].astype(F32)) * inverse
            hid[layer, mine, cols] = jax.nn.gelu(value, approximate=True).astype(BF16)
        launch(hidden_copy, layer)
        launch(hidden_give, layer, cond=lacks(layer))

        @pl.when(core == layer)
        def _():
            hg[z, core_rows] = hid[layer, mine]

        if layer == 0:
            ssq[...] = jnp.zeros_like(ssq)

    def ring_length(k, way):
        return hi if k == way else lo

    def ring_copy(k, way, s, layer):
        delta = 1 if way == 0 else -1
        ref = hg.at[plane_at(-delta * s), block_of(layer if k == 0 else 1 - layer, h2)]
        return remote(
            ref,
            ref,
            h_ss.at[k, way, s],
            h_rs.at[k, way, s],
            {"dp": plane_at(delta) * INNER + q},
        )

    def ring_landing(k, way, d, layer):
        delta = 1 if way == 0 else -1
        ref = hg.at[plane_at(-delta * d), block_of(layer if k == 0 else 1 - layer, h2)]
        return remote(
            ref,
            ref,
            h_ss.at[k, way, d - 1],
            h_rs.at[k, way, d - 1],
            {"dp": plane_at(delta) * INNER + q},
        )

    def ring_step(layer, d):
        @pl.when(core == layer)
        def _():
            for k in range(2):
                if d == 0 and k == 1:
                    hidden_given(layer).wait_recv()
                for way in range(2):
                    length = ring_length(k, way)
                    if 0 < d <= length:
                        ring_landing(k, way, d, layer).wait_recv()
                    if d < length:
                        ring_copy(k, way, d, layer).start()

    def part_copy(layer, block):
        return remote(
            part_send.at[layer, block],
            part_recv.at[layer, t],
            p_ss.at[layer, block],
            p_rs.at[layer, t],
            {"tensor": block},
        )

    def part_landing(layer, tensor):
        ref = part_recv.at[layer, tensor]
        return remote(
            ref, ref, p_ss.at[layer, tensor], p_rs.at[layer, tensor], {"tensor": tensor}
        )

    def down_block(layer, block):
        part_send[layer, block] = jnp.dot(
            hid[layer], wd[layer, block], preferred_element_type=F32
        ).astype(BF16)

        @pl.when(block != t)
        def _():
            part_copy(layer, block).start()

    def next_copy(off):
        ref = xb.at[1, t]
        return remote(ref, ref, x_ss.at[off], x_rs.at[t], {"tensor": tensor_at(off)})

    def next_landing(tensor):
        ref = xb.at[1, tensor]
        return remote(ref, ref, x_ss.at[0], x_rs.at[tensor], {"tensor": tensor})

    def state_copy(layer, away):
        return remote(
            xb.at[layer + 1, t, theirs if away else mine],
            state_buf.at[core_rows, my_cols],
            st_ss.at[layer, away],
            st_rs.at[core, q],
            {"section": layer, "dp": beside} if away else {"section": other},
        )

    def state_landing(from_core, from_class):
        ref = state_buf.at[block_of(from_core, h2), block_of(from_class, feat)]
        return remote(
            ref, ref, st_ss.at[0, 0], st_rs.at[from_core, from_class], {"section": other}
        )

    def finish_down(layer):
        value = xb[layer, t].astype(F32) + part_send[layer, t].astype(F32)
        for off in range(1, nt):
            tensor = tensor_at(off)
            part_landing(layer, tensor).wait_recv()
            value = value + part_recv[layer, tensor].astype(F32)
        xb[layer + 1, t] = value.astype(BF16)
        if layer == 0:
            for off in far_first(nt):
                launch(next_copy, off)
        launch(state_copy, layer, 1)
        launch(state_copy, layer, 0, cond=lacks(layer))

        @pl.when(core == layer)
        def _():
            state_buf[core_rows, my_cols] = xb[layer + 1, t, mine]

    def grad_block(origin, first=False):
        left = hg[origin]
        for index, cols in ((0, their_cols), (1, my_cols)):
            value = lax.dot_general(
                left, cb[origin, :, cols], (((0,), (0,)), ((), ())), preferred_element_type=F32
            )
            gacc[index] = value if first else gacc[index] + value

    def grad_copy():
        return remote(gsend, grecv, gx_ss.at[0], gx_rs.at[0], {"dp": beside})

    advance(0, 1)
    if hi >= 2:
        advance(0, 2)
    for off in range(nt):
        tensor = tensor_at(off)
        token_landing(tensor, 1 - q).wait_recv()
        if off:
            token_landing(tensor, q).wait_recv()
            gain_landing(core, tensor).wait_recv()
        gain_landing(other, tensor).wait_recv()

    def prepare_first(block, carry):
        prepare(0, block)
        return carry

    lax.fori_loop(0, nt, prepare_first, 0)
    send_sums(0)
    share_cotangent()

    def use_near(m, d, use):
        use(along(d))
        take(m, d)
        use(against(d))

    def use_far(m, use):
        take_far(m)
        use(along(hi))

    up0 = functools.partial(up_block, 0)
    up_block(0, z, first=True)
    if lo >= 1:
        use_near(0, 1, up0)
    for d in range(3, hi + 1):
        advance(0, d)
        if d == hi:
            advance(1, 0)
        use_near(0, d - 1, up0)
    if hi < 3:
        advance(1, 0)
        for d in range(2, lo + 1):
            use_near(0, d, up0)
    use_far(0, up0)
    send_up(0)
    if hi >= 2:
        advance(1, 1)
    finish_up(0)
    for d in range(2, hi):
        advance(1, d)
    advance(2, 0)
    down0 = functools.partial(down_block, 0)
    hidden_landing(0).wait_recv()
    down_block(0, z)
    for d in range(1, lo):
        use_near(1, d, down0)
    advance(1, hi)
    if lo >= 1:
        use_near(1, lo, down0)
    use_far(1, down0)
    advance(2, 1)
    ring_step(0, 0)
    if hi >= 2:
        advance(2, 2)
    finish_down(0)
    ring_step(0, 1)
    for d in range(3, hi + 1):
        advance(2, d)
    advance(3, 0)
    for d in range(2, hi + 1):
        ring_step(0, d)

    prepare(1, t)
    for d in range(1, lo + 1):
        take(2, d)
    take_far(2)
    up_block(1, t, first=True)
    for count, off in enumerate(reversed(far_first(nt))):
        if count == nt // 2 - 1:
            advance(3, 1)
        tensor = tensor_at(off)
        next_landing(tensor).wait_recv()
        prepare(1, tensor)
        up_block(1, tensor)
    send_sums(1)
    send_up(1)
    if hi >= 2:
        advance(3, 2)
    finish_up(1)
    ring_step(1, 0)
    for d in range(3, hi + 1):
        advance(3, d)
    hidden_landing(1).wait_recv()
    down1 = functools.partial(down_block, 1)
    down_block(1, z)
    for d in range(1, lo + 1):
        use_near(3, d, down1)
    use_far(3, down1)

    for off in range(1, nt):
        cot_share_landing(tensor_at(off)).wait_recv()

    grad_block(z, first=True)
    for d in range(1, hi + 1):
        ring_step(1, d)
        if d <= lo:

            def both(i, carry):
                grad_block(plane_at(d - 2 * d * i))
                return carry

            lax.fori_loop(0, 2, both, 0)
        else:
            grad_block(plane_at(d))
    gsend[...] = gacc[0].astype(BF16)
    grad_copy().start()
    finish_down(1)
    state_landing(other, q).wait_recv()
    state_landing(core, 1 - q).wait_recv()
    state_landing(other, 1 - q).wait_recv()
    state_store = pltpu.make_async_copy(state_buf, state_out, end_sem.at[0])
    state_store.start()
    grad_copy().wait_recv()
    grad_copy().wait_send()
    gsend[...] = (gacc[1] + grecv[...].astype(F32)).astype(BF16)
    grad_store = pltpu.make_async_copy(gsend, grad_out, end_sem.at[1])
    grad_store.start()

    for make, cond in sends:
        if cond is None:
            make().wait_send()
        else:
            pl.when(cond())(lambda: make().wait_send())
    for layer in range(sections):
        for block in range(nt):

            @pl.when(block != t)
            def _():
                part_copy(layer, block).wait_send()

    for k in range(2):
        for way in range(2):
            for s in range(ring_length(k, way)):
                ring_copy(k, way, s, core).wait_send()
    state_store.wait()
    grad_store.wait()


def stack(sizes, tokens, gain, w_up, w_down, cotangent):
    sections, dp_count, nt = sizes
    nz = dp_count // INNER
    assert sections == 2 and nz == nt and nz % 2 == 0
    rows, slice_width = tokens.shape
    feat = slice_width // INNER
    h2 = rows // sections
    hidden = w_up.shape[2]
    assert w_up.shape[1] == feat and w_down.shape[2] == feat
    width = slice_width * nt
    hi = nz // 2
    dma = pltpu.SemaphoreType.DMA
    hbm = pl.BlockSpec(memory_space=pl.ANY)
    vmem = pl.BlockSpec(memory_space=pltpu.VMEM)

    def buf(*dims, dtype=BF16):
        return pltpu.VMEM(dims, dtype)

    def pair(*dims):
        return [dma(dims)] * 2

    return pl.pallas_call(
        functools.partial(stack_kernel, sizes, width),
        name="stack",
        out_shape=(
            jax.ShapeDtypeStruct((rows, slice_width), BF16),
            jax.ShapeDtypeStruct((hidden, feat), BF16),
        ),
        in_specs=[hbm, vmem, hbm, hbm, hbm],
        out_specs=(hbm, hbm),
        scratch_shapes=[
            buf(rows, slice_width),
            buf(1, slice_width, dtype=F32),
            buf(sections, nt, 1, feat, dtype=F32),
            buf(sections, nz, feat, hidden),
            buf(sections, nz, hidden, feat),
            buf(sections + 1, nt, rows, feat),
            buf(nt, rows, feat),
            buf(rows, LANES, dtype=F32),
            buf(rows, hidden, dtype=F32),
            buf(sections, h2, LANES, dtype=F32),
            buf(sections, h2, LANES, dtype=F32),
            buf(sections, h2, hidden),
            buf(sections, h2, hidden),
            buf(sections, rows, hidden),
            buf(sections, nt, rows, feat),
            buf(sections, nt, rows, feat),
            buf(rows, slice_width),
            buf(nz, rows, hidden),
            buf(nz, rows, slice_width),
            buf(2, hidden, feat, dtype=F32),
            buf(hidden, feat),
            buf(hidden, feat),
            dma((4,)),
            dma((2, nt)),
            dma((nt, INNER)),
            dma((2, nt)),
            dma((sections, nt)),
        ]
        + pair(2 * sections, PIECES, hi)
        + pair(2 * sections, PIECES, hi + 1)
        + pair(nz)
        + pair(nt)
        + pair(sections) * 4
        + pair(2, 2, hi)
        + pair(sections, nt)
        + pair(nt)
        + [dma((sections, 2)), dma((sections, INNER))]
        + pair(1)
        + [dma((2,))],
        compiler_params=pltpu.CompilerParams(collective_id=0, has_side_effects=True),
    )(tokens, gain, w_up, w_down, cotangent)


def body(tokens, gain, w_up, w_down, cotangent):
    sizes = (lax.axis_size("section"), lax.axis_size("dp"), lax.axis_size("tensor"))
    state, grad = stack(sizes, tokens, gain, w_up, w_down, cotangent)
    return (state[None], grad[None])


def solution(mesh):
    placed = (
        P("dp", "tensor"),
        P("section", "tensor"),
        P("section", "dp", "tensor"),
        P("section", "tensor", "dp"),
        P("section", "dp", None),
    )
    return jax.shard_map(
        body,
        mesh=mesh,
        in_specs=placed,
        out_specs=(P("section", "dp", "tensor"), P("section", "tensor", "dp")),
        check_vma=False,
    )
```

```python
import functools

import jax
import jax.numpy as jnp
from jax import lax
from jax.experimental import pallas as pl
from jax.experimental.pallas import tpu as pltpu
from jax.sharding import PartitionSpec as P

EPS = 1e-06
F32 = jnp.float32
BF16 = jnp.bfloat16

MESH = pl.DeviceIdType.MESH
LANES = 128
PIECES = 4
INNER = 2


def far_first(count):
    return sorted(range(1, count), key=lambda k: abs(2 * k - count))


def remote(src, dst, send_sem, recv_sem, target):
    return pltpu.make_async_remote_copy(
        src_ref=src,
        dst_ref=dst,
        send_sem=send_sem,
        recv_sem=recv_sem,
        device_id=target,
        device_id_type=MESH,
    )


def stack_kernel(
    sizes,
    width,
    tok_ref,
    gain_ref,
    up_ref,
    down_ref,
    cot_ref,
    state_out,
    grad_out,
    tok,
    gain_f,
    gains,
    wu,
    wd,
    xb,
    xg,
    ssq,
    acc,
    sq_send,
    sq_recv,
    up_send,
    up_recv,
    hid,
    part_send,
    part_recv,
    state_buf,
    hg,
    cb,
    gacc,
    gsend,
    grecv,
    ld,
    tk_ss,
    tk_rs,
    ga_ss,
    ga_rs,
    z_ss,
    z_rs,
    f_ss,
    f_rs,
    c_ss,
    c_rs,
    cs_ss,
    cs_rs,
    sq_ss,
    sq_rs,
    ux_ss,
    ux_rs,
    ax_ss,
    ax_rs,
    hd_ss,
    hd_rs,
    h_ss,
    h_rs,
    p_ss,
    p_rs,
    x_ss,
    x_rs,
    st_ss,
    st_rs,
    gx_ss,
    gx_rs,
    end_sem,
):
    sections, dp_count, nt = sizes
    nz = dp_count // INNER
    hi = nz // 2
    lo = nz - 1 - hi
    rows, slice_width = tok.shape
    h2 = rows // sections
    feat = slice_width // INNER
    part_rows = rows // nt
    hidden = wu.shape[3]

    core = lax.axis_index("section")
    t = lax.axis_index("tensor")
    me = lax.axis_index("dp")
    z = me // INNER
    q = lax.rem(me, INNER)
    other = 1 - core
    sign = 1 - 2 * core
    beside = z * INNER + 1 - q

    def block_of(index, size):
        if isinstance(index, int):
            return pl.ds(index * size, size)
        return pl.ds(pl.multiple_of(index * size, size), size)

    mine = block_of(q, h2)
    theirs = block_of(1 - q, h2)
    core_rows = block_of(core, h2)
    other_rows = block_of(other, h2)
    my_cols = block_of(q, feat)
    their_cols = block_of(1 - q, feat)
    my_part = block_of(t, part_rows)

    def tensor_at(off):
        return lax.rem(t + off, nt)

    def plane_at(shift):
        return lax.rem(z + nz + shift, nz)

    sends = []

    def launch(make, *args, cond=None):
        make = functools.partial(make, *args)
        sends.append((make, cond))
        if cond is None:
            make().start()
        else:
            pl.when(cond())(lambda: make().start())

    loads = [
        pltpu.make_async_copy(up_ref.at[0], wu.at[core, z], ld.at[0]),
        pltpu.make_async_copy(tok_ref, tok, ld.at[1]),
        pltpu.make_async_copy(down_ref.at[0], wd.at[core, z], ld.at[2]),
        pltpu.make_async_copy(
            cot_ref.at[0, my_part, block_of(z, slice_width)], cb.at[z, my_part], ld.at[3]
        ),
    ]
    for copy in loads:
        copy.start()

    barrier = pltpu.get_barrier_semaphore()

    def greet(target):
        pl.semaphore_signal(barrier, inc=1, device_id=target, device_id_type=MESH)

    for m in far_first(nz):
        greet({"dp": plane_at(m) * INNER + q})
    for off in far_first(nt) + [0]:
        greet({"dp": beside, "tensor": tensor_at(off)})
        greet({"section": other, "tensor": tensor_at(off)})
        if off:
            greet({"tensor": tensor_at(off)})
    greet({"section": other, "dp": beside})

    gain_f[...] = gain_ref[...].astype(F32)
    gains[core, t] = gain_f[:, my_cols]
    ssq[...] = jnp.zeros_like(ssq)
    for copy in loads:
        copy.wait()
    xb[0, t, mine] = tok[core_rows, my_cols]

    pl.semaphore_wait(barrier, (nz - 1) + (2 * nt - 1) + nt + 1)

    def weight(layer, kind, origin, piece):
        buf = wd if kind else wu
        return buf.at[layer, origin, block_of(piece, buf.shape[2] // PIECES)]

    def along(d):
        return plane_at(-sign * d)

    def against(d):
        return plane_at(sign * d)

    def hop(m, piece, s):
        ref = weight(m // 2, m % 2, along(s), piece)
        return remote(
            ref,
            ref,
            z_ss.at[m, piece, s],
            z_rs.at[m, piece, s],
            {"dp": plane_at(sign) * INNER + q},
        )

    def landing(m, piece, d):
        ref = weight(m // 2, m % 2, along(d), piece)
        return remote(
            ref,
            ref,
            z_ss.at[m, piece, d - 1],
            z_rs.at[m, piece, d - 1],
            {"dp": plane_at(sign) * INNER + q},
        )

    def push(m, piece, d):
        ref = weight(m // 2, m % 2, along(d), piece)
        return remote(
            ref, ref, f_ss.at[m, piece, d], f_rs.at[m, piece, d], {"section": other}
        )

    def pushed(m, piece, d):
        ref = weight(m // 2, m % 2, against(d), piece)
        return remote(
            ref, ref, f_ss.at[m, piece, d], f_rs.at[m, piece, d], {"section": other}
        )

    def push_own(kind, piece):
        ref = weight(core, kind, z, piece)
        m = 2 * core + kind
        return remote(
            ref, ref, f_ss.at[m, piece, 0], f_rs.at[m, piece, 0], {"section": other}
        )

    def lacks(layer):
        return lambda: core != layer

    half = PIECES // 2
    far_pieces = [core * half + j for j in range(half)]
    near_pieces = [other * half + j for j in range(half)]

    def begin(m):
        for piece in range(PIECES):

            @pl.when(core != m // 2)
            def _():
                pushed(m, piece, 0).wait_recv()

        for piece in range(PIECES) if lo else far_pieces:
            launch(hop, m, piece, 0)

    def advance(m, d):
        for piece in range(PIECES) if d < lo else far_pieces:
            landing(m, piece, d).wait_recv()
            if d < hi:
                launch(hop, m, piece, d)
            launch(push, m, piece, d)
        if d == max(lo, 1) and m + 1 < 2 * sections:
            begin(m + 1)
        if d == lo:
            for piece in near_pieces:
                landing(m, piece, d).wait_recv()
                launch(push, m, piece, d)

    rounds = [(m, d) for m in range(2 * sections) for d in range(1, hi + 1)]
    done_rounds = [0]

    def z_until(m, d):
        last = rounds.index((m, min(d, hi))) + 1
        for r in range(done_rounds[0], last):
            advance(*rounds[r])
        done_rounds[0] = max(done_rounds[0], last)

    def take(m, d):
        for piece in range(PIECES):
            pushed(m, piece, d).wait_recv()

    def take_far(m):
        for piece in near_pieces:
            pushed(m, piece, hi).wait_recv()

    for piece in range(PIECES):
        launch(push_own, 0, piece)

    @pl.when(core == 0)
    def _():
        for piece in range(PIECES) if lo else far_pieces:
            hop(0, piece, 0).start()

    def token_copy(away, off):
        cols, dp = (their_cols, beside) if away else (my_cols, me)
        return remote(
            tok.at[core_rows, cols],
            xb.at[0, t, mine],
            tk_ss.at[away, off],
            tk_rs.at[t, q],
            {"dp": dp, "tensor": tensor_at(off)},
        )

    def token_landing(tensor, cls):
        ref = xb.at[0, tensor, block_of(cls, h2)]
        return remote(ref, ref, tk_ss.at[0, 0], tk_rs.at[tensor, cls], {"dp": beside})

    for off in far_first(nt) + [0]:
        launch(token_copy, 1, off)
        if off:
            launch(token_copy, 0, off)

    def gain_copy(away, off):
        return remote(
            gains.at[core, t],
            gains.at[core, t],
            ga_ss.at[away, off],
            ga_rs.at[core, t],
            {"section": other if away else core, "tensor": tensor_at(off)},
        )

    def gain_landing(layer, tensor):
        ref = gains.at[layer, tensor]
        return remote(ref, ref, ga_ss.at[0, 0], ga_rs.at[layer, tensor], {"section": other})

    for off in far_first(nt) + [0]:
        launch(gain_copy, 1, off)
        if off:
            launch(gain_copy, 0, off)
    for piece in range(PIECES):
        launch(push_own, 1, piece)

    def cot_copy(m):
        to = plane_at(m)
        return remote(
            cot_ref.at[0, my_part, block_of(to, slice_width)],
            cb.at[z, my_part],
            c_ss.at[m],
            c_rs.at[z],
            {"dp": to * INNER + q},
        )

    def cot_landing(origin):
        ref = cb.at[origin, my_part]
        return remote(ref, ref, c_ss.at[0], c_rs.at[origin], {"dp": beside})

    @pl.when(core != 0)
    def _():
        for piece in range(PIECES):
            pushed(0, piece, 0).wait_recv()
        for piece in range(PIECES) if lo else far_pieces:
            hop(0, piece, 0).start()

    for piece in range(PIECES) if lo else far_pieces:
        sends.append((functools.partial(hop, 0, piece, 0), None))
    for m in far_first(nz):
        launch(cot_copy, m)

    def cot_share(off):
        ref = cb.at[:, my_part]
        return remote(ref, ref, cs_ss.at[off], cs_rs.at[t], {"tensor": tensor_at(off)})

    def cot_share_landing(tensor):
        ref = cb.at[:, block_of(tensor, part_rows)]
        return remote(ref, ref, cs_ss.at[0], cs_rs.at[tensor], {"dp": beside})

    def await_cotangent():
        for m in range(1, nz):
            cot_landing(plane_at(m)).wait_recv()

    def share_cotangent(first, last):
        for off in far_first(nt)[first:last]:
            launch(cot_share, off)

    def prepare(layer, block):
        x = xb[layer, block].astype(F32)
        xg[block] = (x * gains[layer, block]).astype(BF16)
        square = x * x
        total = ssq[...]
        for lower in range(0, feat, LANES):
            total = total + square[:, lower : lower + LANES]
        ssq[...] = total

    def up_block(layer, block, first=False):
        value = jnp.dot(xg[block], wu[layer, block], preferred_element_type=F32)
        acc[...] = value if first else acc[...] + value

    def sum_copy(layer):
        return remote(
            sq_send.at[layer], sq_recv.at[layer], sq_ss.at[layer], sq_rs.at[layer], {"dp": beside}
        )

    def send_sums(layer):
        sq_send[layer] = jnp.broadcast_to(
            jnp.sum(ssq[theirs], axis=1, keepdims=True), (h2, LANES)
        )
        launch(sum_copy, layer)

    def up_copy(layer):
        return remote(
            up_send.at[layer], up_recv.at[layer], ux_ss.at[layer], ux_rs.at[layer], {"dp": beside}
        )

    def send_up(layer):
        up_send[layer] = acc[theirs].astype(BF16)
        launch(up_copy, layer)

    def hidden_copy(layer):
        ref = hid.at[layer, mine]
        return remote(ref, ref, ax_ss.at[layer], ax_rs.at[layer], {"dp": beside})

    def hidden_landing(layer):
        ref = hid.at[layer, theirs]
        return remote(ref, ref, ax_ss.at[layer], ax_rs.at[layer], {"dp": beside})

    def hidden_give(layer):
        return remote(
            hid.at[layer, mine],
            hg.at[z, core_rows],
            hd_ss.at[layer],
            hd_rs.at[layer],
            {"section": other},
        )

    def hidden_given(layer):
        ref = hg.at[z, other_rows]
        return remote(ref, ref, hd_ss.at[layer], hd_rs.at[layer], {"section": other})

    def finish_up(layer):
        sum_copy(layer).wait_recv()
        total = jnp.sum(ssq[mine], axis=1, keepdims=True) + sq_recv[layer]
        inverse = lax.rsqrt(total / width + EPS)
        up_copy(layer).wait_recv()
        for lower in range(0, hidden, LANES):
            cols = pl.ds(lower, LANES)
            value = (acc[mine, cols] + up_recv[layer, :, cols].astype(F32)) * inverse
            hid[layer, mine, cols] = jax.nn.gelu(value, approximate=True).astype(BF16)
        launch(hidden_copy, layer)
        launch(hidden_give, layer, cond=lacks(layer))

        @pl.when(core == layer)
        def _():
            hg[z, core_rows] = hid[layer, mine]

        if layer == 0:
            ssq[...] = jnp.zeros_like(ssq)

    def ring_length(k, way):
        return hi if k == way else lo

    def ring_copy(k, way, s, layer):
        delta = 1 if way == 0 else -1
        ref = hg.at[plane_at(-delta * s), block_of(layer if k == 0 else 1 - layer, h2)]
        return remote(
            ref,
            ref,
            h_ss.at[k, way, s],
            h_rs.at[k, way, s],
            {"dp": plane_at(delta) * INNER + q},
        )

    def ring_landing(k, way, d, layer):
        delta = 1 if way == 0 else -1
        ref = hg.at[plane_at(-delta * d), block_of(layer if k == 0 else 1 - layer, h2)]
        return remote(
            ref,
            ref,
            h_ss.at[k, way, d - 1],
            h_rs.at[k, way, d - 1],
            {"dp": plane_at(delta) * INNER + q},
        )

    def ring_step(layer, d):
        @pl.when(core == layer)
        def _():
            for k in range(2):
                if d == 0 and k == 1:
                    hidden_given(layer).wait_recv()
                for way in range(2):
                    length = ring_length(k, way)
                    if 0 < d <= length:
                        ring_landing(k, way, d, layer).wait_recv()
                    if d < length:
                        ring_copy(k, way, d, layer).start()

    def part_copy(layer, block):
        return remote(
            part_send.at[layer, block],
            part_recv.at[layer, t],
            p_ss.at[layer, block],
            p_rs.at[layer, t],
            {"tensor": block},
        )

    def part_landing(layer, tensor):
        ref = part_recv.at[layer, tensor]
        return remote(
            ref, ref, p_ss.at[layer, tensor], p_rs.at[layer, tensor], {"tensor": tensor}
        )

    def down_block(layer, block):
        part_send[layer, block] = jnp.dot(
            hid[layer], wd[layer, block], preferred_element_type=F32
        ).astype(BF16)

        @pl.when(block != t)
        def _():
            part_copy(layer, block).start()

    def next_copy(off):
        ref = xb.at[1, t]
        return remote(ref, ref, x_ss.at[off], x_rs.at[t], {"tensor": tensor_at(off)})

    def next_landing(tensor):
        ref = xb.at[1, tensor]
        return remote(ref, ref, x_ss.at[0], x_rs.at[tensor], {"tensor": tensor})

    def state_copy(layer, away):
        return remote(
            xb.at[layer + 1, t, theirs if away else mine],
            state_buf.at[core_rows, my_cols],
            st_ss.at[layer, away],
            st_rs.at[core, q],
            {"section": layer, "dp": beside} if away else {"section": other},
        )

    def state_landing(from_core, from_class):
        ref = state_buf.at[block_of(from_core, h2), block_of(from_class, feat)]
        return remote(
            ref, ref, st_ss.at[0, 0], st_rs.at[from_core, from_class], {"section": other}
        )

    def finish_down(layer):
        value = xb[layer, t].astype(F32) + part_send[layer, t].astype(F32)
        for off in range(1, nt):
            tensor = tensor_at(off)
            part_landing(layer, tensor).wait_recv()
            value = value + part_recv[layer, tensor].astype(F32)
        xb[layer + 1, t] = value.astype(BF16)
        if layer == 0:
            for off in far_first(nt):
                launch(next_copy, off)
        launch(state_copy, layer, 1)
        launch(state_copy, layer, 0, cond=lacks(layer))

        @pl.when(core == layer)
        def _():
            state_buf[core_rows, my_cols] = xb[layer + 1, t, mine]

    def grad_block(origin, first=False):
        left = hg[origin]
        for index, cols in ((0, their_cols), (1, my_cols)):
            value = lax.dot_general(
                left, cb[origin, :, cols], (((0,), (0,)), ((), ())), preferred_element_type=F32
            )
            gacc[index] = value if first else gacc[index] + value

    def grad_copy():
        return remote(gsend, grecv, gx_ss.at[0], gx_rs.at[0], {"dp": beside})

    z_until(0, 2)
    for off in range(nt):
        tensor = tensor_at(off)
        token_landing(tensor, 1 - q).wait_recv()
        if off:
            token_landing(tensor, q).wait_recv()
            gain_landing(core, tensor).wait_recv()
        gain_landing(other, tensor).wait_recv()

    def prepare_first(block, carry):
        prepare(0, block)
        return carry

    lax.fori_loop(0, nt, prepare_first, 0)
    send_sums(0)

    def use_near(m, d, use):
        use(along(d))
        take(m, d)
        use(against(d))

    def use_far(m, use):
        take_far(m)
        use(along(hi))

    up0 = functools.partial(up_block, 0)
    up_block(0, z, first=True)
    for d in range(1, lo + 1):
        z_until(0, d + 1)
        use_near(0, d, up0)
    z_until(0, hi)
    use_far(0, up0)
    send_up(0)
    await_cotangent()
    z_until(1, 1)
    finish_up(0)
    share_cotangent(0, nt // 2 - 1)
    z_until(1, hi)
    down0 = functools.partial(down_block, 0)
    hidden_landing(0).wait_recv()
    down_block(0, z)
    for d in range(1, lo + 1):
        use_near(1, d, down0)
    use_far(1, down0)
    ring_step(0, 0)
    z_until(2, 1)
    if hi > 1:
        ring_step(0, 1)
    z_until(2, 2)
    if hi > 2:
        ring_step(0, 2)
    finish_down(0)
    share_cotangent(nt // 2 - 1, nt)
    z_until(2, 3)
    if hi > 3:
        ring_step(0, 3)
    z_until(2, hi)
    for d in range(max(1, min(4, hi)), hi + 1):
        ring_step(0, d)

    prepare(1, t)
    for d in range(1, lo + 1):
        take(2, d)
    take_far(2)
    up_block(1, t, first=True)
    for off in reversed(far_first(nt)):
        tensor = tensor_at(off)
        next_landing(tensor).wait_recv()
        prepare(1, tensor)
        up_block(1, tensor)
    send_sums(1)
    send_up(1)
    z_until(3, 1)
    for off in range(1, nt):
        cot_share_landing(tensor_at(off)).wait_recv()

    @pl.when(core == 0)
    def _():
        grad_block(z, first=True)

        def one(i, carry):
            grad_block(plane_at(i))
            return carry

        lax.fori_loop(1, nz, one, 0)
        gsend[...] = gacc[0].astype(BF16)

    z_until(3, 2)
    finish_up(1)
    pl.when(core == 0)(lambda: grad_copy().start())
    ring_step(1, 0)
    z_until(3, hi)
    if hi > 1:
        ring_step(1, 1)
    hidden_landing(1).wait_recv()
    down1 = functools.partial(down_block, 1)
    down_block(1, z)
    for d in range(1, lo + 1):
        use_near(3, d, down1)
    use_far(3, down1)

    def grad_step(d):
        if d == 0:
            grad_block(z, first=True)
        elif d <= lo:

            def both(i, carry):
                grad_block(plane_at(d - 2 * d * i))
                return carry

            lax.fori_loop(0, 2, both, 0)
        else:
            grad_block(plane_at(d))

    middle = max(1, hi // 2)

    @pl.when(core == 1)
    def _():
        for d in range(middle + 1):
            if d > 1 or d == hi:
                ring_step(1, d)
            grad_step(d)

    finish_down(1)

    @pl.when(core == 1)
    def _():
        for d in range(middle + 1, hi + 1):
            ring_step(1, d)
            grad_step(d)
        gsend[...] = gacc[0].astype(BF16)
        grad_copy().start()

    state_landing(other, q).wait_recv()
    state_landing(core, 1 - q).wait_recv()
    state_landing(other, 1 - q).wait_recv()
    state_store = pltpu.make_async_copy(state_buf, state_out, end_sem.at[0])
    state_store.start()
    grad_copy().wait_recv()
    grad_copy().wait_send()
    gsend[...] = (gacc[1] + grecv[...].astype(F32)).astype(BF16)
    grad_store = pltpu.make_async_copy(gsend, grad_out, end_sem.at[1])
    grad_store.start()

    for make, cond in sends:
        if cond is None:
            make().wait_send()
        else:
            pl.when(cond())(lambda: make().wait_send())
    for layer in range(sections):
        for block in range(nt):

            @pl.when(block != t)
            def _():
                part_copy(layer, block).wait_send()

    for k in range(2):
        for way in range(2):
            for s in range(ring_length(k, way)):
                ring_copy(k, way, s, core).wait_send()
    state_store.wait()
    grad_store.wait()


def stack(sizes, tokens, gain, w_up, w_down, cotangent):
    sections, dp_count, nt = sizes
    nz = dp_count // INNER
    assert sections == 2 and nz == nt and nz % 2 == 0
    rows, slice_width = tokens.shape
    feat = slice_width // INNER
    h2 = rows // sections
    hidden = w_up.shape[2]
    assert w_up.shape[1] == feat and w_down.shape[2] == feat
    width = slice_width * nt
    hi = nz // 2
    dma = pltpu.SemaphoreType.DMA
    hbm = pl.BlockSpec(memory_space=pl.ANY)
    vmem = pl.BlockSpec(memory_space=pltpu.VMEM)

    def buf(*dims, dtype=BF16):
        return pltpu.VMEM(dims, dtype)

    def pair(*dims):
        return [dma(dims)] * 2

    return pl.pallas_call(
        functools.partial(stack_kernel, sizes, width),
        name="stack",
        out_shape=(
            jax.ShapeDtypeStruct((rows, slice_width), BF16),
            jax.ShapeDtypeStruct((hidden, feat), BF16),
        ),
        in_specs=[hbm, vmem, hbm, hbm, hbm],
        out_specs=(hbm, hbm),
        scratch_shapes=[
            buf(rows, slice_width),
            buf(1, slice_width, dtype=F32),
            buf(sections, nt, 1, feat, dtype=F32),
            buf(sections, nz, feat, hidden),
            buf(sections, nz, hidden, feat),
            buf(sections + 1, nt, rows, feat),
            buf(nt, rows, feat),
            buf(rows, LANES, dtype=F32),
            buf(rows, hidden, dtype=F32),
            buf(sections, h2, LANES, dtype=F32),
            buf(sections, h2, LANES, dtype=F32),
            buf(sections, h2, hidden),
            buf(sections, h2, hidden),
            buf(sections, rows, hidden),
            buf(sections, nt, rows, feat),
            buf(sections, nt, rows, feat),
            buf(rows, slice_width),
            buf(nz, rows, hidden),
            buf(nz, rows, slice_width),
            buf(2, hidden, feat, dtype=F32),
            buf(hidden, feat),
            buf(hidden, feat),
            dma((4,)),
            dma((2, nt)),
            dma((nt, INNER)),
            dma((2, nt)),
            dma((sections, nt)),
        ]
        + pair(2 * sections, PIECES, hi)
        + pair(2 * sections, PIECES, hi + 1)
        + pair(nz)
        + pair(nt)
        + pair(sections) * 4
        + pair(2, 2, hi)
        + pair(sections, nt)
        + pair(nt)
        + [dma((sections, 2)), dma((sections, INNER))]
        + pair(1)
        + [dma((2,))],
        compiler_params=pltpu.CompilerParams(collective_id=0, has_side_effects=True),
    )(tokens, gain, w_up, w_down, cotangent)


def body(tokens, gain, w_up, w_down, cotangent):
    sizes = (lax.axis_size("section"), lax.axis_size("dp"), lax.axis_size("tensor"))
    state, grad = stack(sizes, tokens, gain, w_up, w_down, cotangent)
    return (state[None], grad[None])


def solution(mesh):
    placed = (
        P("dp", "tensor"),
        P("section", "tensor"),
        P("section", "dp", "tensor"),
        P("section", "tensor", "dp"),
        P("section", "dp", None),
    )
    return jax.shard_map(
        body,
        mesh=mesh,
        in_specs=placed,
        out_specs=(P("section", "dp", "tensor"), P("section", "tensor", "dp")),
        check_vma=False,
    )
```

```python
import functools

import jax
import jax.numpy as jnp
from jax import lax
from jax.experimental import pallas as pl
from jax.experimental.pallas import tpu as pltpu
from jax.sharding import PartitionSpec as P

EPS = 1e-06
F32 = jnp.float32
BF16 = jnp.bfloat16

MESH = pl.DeviceIdType.MESH
LANES = 128
PIECES = 4
INNER = 2


def far_first(count):
    return sorted(range(1, count), key=lambda k: abs(2 * k - count))


def remote(src, dst, send_sem, recv_sem, target):
    return pltpu.make_async_remote_copy(
        src_ref=src,
        dst_ref=dst,
        send_sem=send_sem,
        recv_sem=recv_sem,
        device_id=target,
        device_id_type=MESH,
    )


def stack_kernel(
    sizes,
    width,
    tok_ref,
    gain_ref,
    up_ref,
    down_ref,
    cot_ref,
    state_out,
    grad_out,
    tok,
    gain_f,
    gains,
    wu,
    wd,
    xb,
    xg,
    ssq,
    acc,
    sq_send,
    sq_recv,
    up_send,
    up_recv,
    hid,
    part_send,
    part_recv,
    state_buf,
    hg,
    cb,
    gacc,
    gsend,
    grecv,
    send_sem,
    load_sem,
    tk_rs,
    ga_rs,
    z_rs,
    f_rs,
    c_rs,
    cs_rs,
    sq_rs,
    ux_rs,
    ax_rs,
    hd_rs,
    h_rs,
    p_rs,
    x_rs,
    st_rs,
    gx_rs,
    end_sem,
):
    sections, dp_count, nt = sizes
    nz = dp_count // INNER
    hi = nz // 2
    lo = nz - 1 - hi
    rows, slice_width = tok.shape
    h2 = rows // sections
    feat = slice_width // INNER
    part_rows = rows // nt
    hidden = wu.shape[3]

    core = lax.axis_index("section")
    t = lax.axis_index("tensor")
    me = lax.axis_index("dp")
    z = me // INNER
    q = lax.rem(me, INNER)
    other = 1 - core
    sign = 1 - 2 * core
    beside = z * INNER + 1 - q

    def block_of(index, size):
        if isinstance(index, int):
            return pl.ds(index * size, size)
        return pl.ds(pl.multiple_of(index * size, size), size)

    mine = block_of(q, h2)
    theirs = block_of(1 - q, h2)
    core_rows = block_of(core, h2)
    other_rows = block_of(other, h2)
    my_cols = block_of(q, feat)
    their_cols = block_of(1 - q, feat)
    my_part = block_of(t, part_rows)

    hops, pushes, others, gain_sends, grad_sends = (send_sem.at[i] for i in range(5))

    def bytes_of(*dims, size=2):
        count = size
        for dim in dims:
            count *= dim
        return count

    def await_bytes(sem, count):
        ref = wd.at[pl.ds(0, count // (2 * feat))]
        pltpu.make_async_copy(ref, ref, sem).wait()

    def down_rows(layer, origin, piece=0, pieces=1):
        return block_of((layer * nz + origin) * pieces + piece, hidden // pieces)

    def tensor_at(off):
        return lax.rem(t + off, nt)

    def plane_at(shift):
        return lax.rem(z + nz + shift, nz)

    def launch(make, *args, cond=None):
        if cond is None:
            make(*args).start()
        else:
            pl.when(cond())(lambda: make(*args).start())

    loads = [
        pltpu.make_async_copy(up_ref.at[0], wu.at[core, z], load_sem.at[0]),
        pltpu.make_async_copy(tok_ref, tok, load_sem.at[0]),
        pltpu.make_async_copy(down_ref.at[0], wd.at[down_rows(core, z)], load_sem.at[0]),
        pltpu.make_async_copy(
            cot_ref.at[0, my_part, block_of(z, slice_width)], cb.at[z, my_part], load_sem.at[0]
        ),
    ]
    for copy in loads:
        copy.start()

    barrier = pltpu.get_barrier_semaphore()

    def greet(target):
        pl.semaphore_signal(barrier, inc=1, device_id=target, device_id_type=MESH)

    for m in far_first(nz):
        greet({"dp": plane_at(m) * INNER + q})
    for off in far_first(nt) + [0]:
        greet({"dp": beside, "tensor": tensor_at(off)})
        greet({"section": other, "tensor": tensor_at(off)})
        if off:
            greet({"tensor": tensor_at(off)})
    greet({"section": other, "dp": beside})

    gain_f[...] = gain_ref[...].astype(F32)
    gains[core * nt + t] = gain_f[:, my_cols]
    ssq[...] = jnp.zeros_like(ssq)
    await_bytes(
        load_sem.at[0],
        bytes_of(2, feat, hidden) + bytes_of(rows, slice_width) + bytes_of(part_rows, slice_width),
    )
    xb[0, t, mine] = tok[core_rows, my_cols]

    pl.semaphore_wait(barrier, (nz - 1) + (2 * nt - 1) + nt + 1)

    def weight(layer, kind, origin, piece, pieces=PIECES):
        if kind:
            return wd.at[down_rows(layer, origin, piece, pieces)]
        return wu.at[layer, origin, block_of(piece, feat // pieces)]

    def along(d):
        return plane_at(-sign * d)

    def against(d):
        return plane_at(sign * d)

    def hop(m, piece, s):
        ref = weight(m // 2, m % 2, along(s), piece)
        return remote(
            ref,
            ref,
            hops,
            z_rs.at[m, piece, s],
            {"dp": plane_at(sign) * INNER + q},
        )

    def landing(m, piece, d):
        ref = weight(m // 2, m % 2, along(d), piece)
        return remote(
            ref,
            ref,
            hops,
            z_rs.at[m, piece, d - 1],
            {"dp": plane_at(sign) * INNER + q},
        )

    def push(m, piece, d):
        ref = weight(m // 2, m % 2, along(d), piece)
        return remote(
            ref, ref, pushes, f_rs.at[m, d], {"section": other}
        )

    def pushed(m, d):
        ref = weight(m // 2, m % 2, against(d), 0, 2 if d == hi else 1)
        return remote(ref, ref, pushes, f_rs.at[m, d], {"section": other})

    def push_own(kind, piece):
        ref = weight(core, kind, z, piece)
        m = 2 * core + kind
        return remote(
            ref, ref, pushes, f_rs.at[m, 0], {"section": other}
        )

    def lacks(layer):
        return lambda: core != layer

    half = PIECES // 2
    far_pieces = [core * half + j for j in range(half)]
    near_pieces = [other * half + j for j in range(half)]

    def begin(m):
        @pl.when(core != m // 2)
        def _():
            pushed(m, 0).wait_recv()

        for piece in range(PIECES) if lo else far_pieces:
            launch(hop, m, piece, 0)

    def advance(m, d):
        for piece in range(PIECES) if d < lo else far_pieces:
            landing(m, piece, d).wait_recv()
            if d < hi:
                launch(hop, m, piece, d)
            launch(push, m, piece, d)
        if d == max(lo, 1) and m + 1 < 2 * sections:
            begin(m + 1)
        if d == lo:
            for piece in near_pieces:
                landing(m, piece, d).wait_recv()
                launch(push, m, piece, d)

    rounds = [(m, d) for m in range(2 * sections) for d in range(1, hi + 1)]
    done_rounds = [0]

    def z_until(m, d):
        last = rounds.index((m, min(d, hi))) + 1
        for r in range(done_rounds[0], last):
            advance(*rounds[r])
        done_rounds[0] = max(done_rounds[0], last)

    def take(m, d):
        pushed(m, d).wait_recv()

    def take_far(m):
        pushed(m, hi).wait_recv()

    for piece in range(PIECES):
        launch(push_own, 0, piece)

    @pl.when(core == 0)
    def _():
        for piece in range(PIECES) if lo else far_pieces:
            hop(0, piece, 0).start()

    def token_copy(away, off):
        cols, dp = (their_cols, beside) if away else (my_cols, me)
        return remote(
            tok.at[core_rows, cols],
            xb.at[0, t, mine],
            others,
            tk_rs.at[0],
            {"dp": dp, "tensor": tensor_at(off)},
        )

    for off in far_first(nt) + [0]:
        launch(token_copy, 1, off)
        if off:
            launch(token_copy, 0, off)

    def gain_copy(away, off):
        return remote(
            gains.at[core * nt + t],
            gains.at[core * nt + t],
            gain_sends,
            ga_rs.at[0],
            {"section": other if away else core, "tensor": tensor_at(off)},
        )

    def await_gains(sem):
        ref = gains.at[pl.ds(0, sections * nt - 1)]
        pltpu.make_async_copy(ref, ref, sem).wait()

    for off in far_first(nt) + [0]:
        launch(gain_copy, 1, off)
        if off:
            launch(gain_copy, 0, off)
    for piece in range(PIECES):
        launch(push_own, 1, piece)

    def cot_copy(m):
        to = plane_at(m)
        return remote(
            cot_ref.at[0, my_part, block_of(to, slice_width)],
            cb.at[z, my_part],
            others,
            c_rs.at[0],
            {"dp": to * INNER + q},
        )

    @pl.when(core != 0)
    def _():
        pushed(0, 0).wait_recv()
        for piece in range(PIECES) if lo else far_pieces:
            hop(0, piece, 0).start()

    for m in far_first(nz):
        launch(cot_copy, m)

    def cot_share(off):
        ref = cb.at[:, my_part]
        return remote(ref, ref, others, cs_rs.at[0], {"tensor": tensor_at(off)})

    def await_cotangent():
        await_bytes(c_rs.at[0], bytes_of(nz - 1, part_rows, slice_width))

    def share_cotangent(first, last):
        for off in far_first(nt)[first:last]:
            launch(cot_share, off)

    def prepare(layer, block):
        x = xb[layer, block].astype(F32)
        xg[block] = (x * gains[layer * nt + block]).astype(BF16)
        square = x * x
        total = ssq[...]
        for lower in range(0, feat, LANES):
            total = total + square[:, lower : lower + LANES]
        ssq[...] = total

    def up_block(layer, block, first=False):
        value = jnp.dot(xg[block], wu[layer, block], preferred_element_type=F32)
        acc[...] = value if first else acc[...] + value

    def sum_copy(layer):
        return remote(
            sq_send.at[layer], sq_recv.at[layer], others, sq_rs.at[layer], {"dp": beside}
        )

    def send_sums(layer):
        sq_send[layer] = jnp.broadcast_to(
            jnp.sum(ssq[theirs], axis=1, keepdims=True), (h2, LANES)
        )
        launch(sum_copy, layer)

    def up_copy(layer):
        return remote(
            up_send.at[layer], up_recv.at[layer], others, ux_rs.at[layer], {"dp": beside}
        )

    def send_up(layer):
        up_send[layer] = acc[theirs].astype(BF16)
        launch(up_copy, layer)

    def hidden_copy(layer):
        ref = hid.at[layer, mine]
        return remote(ref, ref, others, ax_rs.at[layer], {"dp": beside})

    def hidden_landing(layer):
        ref = hid.at[layer, theirs]
        return remote(ref, ref, others, ax_rs.at[layer], {"dp": beside})

    def hidden_give(layer):
        return remote(
            hid.at[layer, mine],
            hg.at[z, core_rows],
            others,
            hd_rs.at[layer],
            {"section": other},
        )

    def hidden_given(layer):
        ref = hg.at[z, other_rows]
        return remote(ref, ref, others, hd_rs.at[layer], {"section": other})

    def finish_up(layer):
        sum_copy(layer).wait_recv()
        total = jnp.sum(ssq[mine], axis=1, keepdims=True) + sq_recv[layer]
        inverse = lax.rsqrt(total / width + EPS)
        up_copy(layer).wait_recv()
        for lower in range(0, hidden, LANES):
            cols = pl.ds(lower, LANES)
            value = (acc[mine, cols] + up_recv[layer, :, cols].astype(F32)) * inverse
            hid[layer, mine, cols] = jax.nn.gelu(value, approximate=True).astype(BF16)
        launch(hidden_copy, layer)
        launch(hidden_give, layer, cond=lacks(layer))

        @pl.when(core == layer)
        def _():
            hg[z, core_rows] = hid[layer, mine]

        if layer == 0:
            ssq[...] = jnp.zeros_like(ssq)

    def ring_length(k, way):
        return hi if k == way else lo

    def ring_copy(k, way, s, layer):
        delta = 1 if way == 0 else -1
        ref = hg.at[plane_at(-delta * s), block_of(layer if k == 0 else 1 - layer, h2)]
        return remote(
            ref,
            ref,
            others,
            h_rs.at[k, way, s],
            {"dp": plane_at(delta) * INNER + q},
        )

    def ring_landing(k, way, d, layer):
        delta = 1 if way == 0 else -1
        ref = hg.at[plane_at(-delta * d), block_of(layer if k == 0 else 1 - layer, h2)]
        return remote(
            ref,
            ref,
            others,
            h_rs.at[k, way, d - 1],
            {"dp": plane_at(delta) * INNER + q},
        )

    def ring_step(layer, d):
        @pl.when(core == layer)
        def _():
            for k in range(2):
                if d == 0 and k == 1:
                    hidden_given(layer).wait_recv()
                for way in range(2):
                    length = ring_length(k, way)
                    if 0 < d <= length:
                        ring_landing(k, way, d, layer).wait_recv()
                    if d < length:
                        ring_copy(k, way, d, layer).start()

    def part_copy(layer, block):
        return remote(
            part_send.at[layer, block],
            part_recv.at[layer, t],
            others,
            p_rs.at[layer],
            {"tensor": block},
        )

    def down_block(layer, block):
        part_send[layer, block] = jnp.dot(
            hid[layer], wd[down_rows(layer, block)], preferred_element_type=F32
        ).astype(BF16)

        @pl.when(block != t)
        def _():
            part_copy(layer, block).start()

    def next_copy(off):
        ref = xb.at[1, t]
        return remote(ref, ref, others, x_rs.at[0], {"tensor": tensor_at(off)})

    def state_copy(layer, away):
        return remote(
            xb.at[layer + 1, t, theirs if away else mine],
            state_buf.at[core_rows, my_cols],
            others,
            st_rs.at[0],
            {"section": layer, "dp": beside} if away else {"section": other},
        )

    def finish_down(layer):
        value = xb[layer, t].astype(F32) + part_send[layer, t].astype(F32)
        await_bytes(p_rs.at[layer], bytes_of(nt - 1, rows, feat))
        for off in range(1, nt):
            value = value + part_recv[layer, tensor_at(off)].astype(F32)
        xb[layer + 1, t] = value.astype(BF16)
        if layer == 0:
            for off in far_first(nt):
                launch(next_copy, off)
        launch(state_copy, layer, 1)
        launch(state_copy, layer, 0, cond=lacks(layer))

        @pl.when(core == layer)
        def _():
            state_buf[core_rows, my_cols] = xb[layer + 1, t, mine]

    def grad_block(origin, first=False):
        left = hg[origin]
        for index, cols in ((0, their_cols), (1, my_cols)):
            value = lax.dot_general(
                left, cb[origin, :, cols], (((0,), (0,)), ((), ())), preferred_element_type=F32
            )
            gacc[index] = value if first else gacc[index] + value

    def grad_copy():
        return remote(gsend, grecv, grad_sends, gx_rs.at[0], {"dp": beside})

    z_until(0, 2)
    await_bytes(tk_rs.at[0], bytes_of(2 * nt - 1, h2, feat))
    await_gains(ga_rs.at[0])

    def prepare_first(block, carry):
        prepare(0, block)
        return carry

    lax.fori_loop(0, nt, prepare_first, 0)
    send_sums(0)

    def use_near(m, d, use):
        use(along(d))
        take(m, d)
        use(against(d))

    def use_far(m, use):
        take_far(m)
        use(along(hi))

    up0 = functools.partial(up_block, 0)
    up_block(0, z, first=True)
    for d in range(1, lo + 1):
        z_until(0, d + 1)
        use_near(0, d, up0)
    z_until(0, hi)
    use_far(0, up0)
    send_up(0)
    await_cotangent()
    z_until(1, 1)
    finish_up(0)
    share_cotangent(0, nt // 2 - 1)
    z_until(1, hi)
    ring_step(0, 0)
    down0 = functools.partial(down_block, 0)
    hidden_landing(0).wait_recv()
    down_block(0, z)
    for d in range(1, lo + 1):
        use_near(1, d, down0)
    use_far(1, down0)
    z_until(2, 1)
    if hi > 1:
        ring_step(0, 1)
    z_until(2, 2)
    finish_down(0)
    share_cotangent(nt // 2 - 1, nt)
    if hi > 2:
        ring_step(0, 2)
    z_until(2, hi)

    prepare(1, t)
    for d in range(1, lo + 1):
        take(2, d)
    take_far(2)
    up_block(1, t, first=True)
    z_until(3, 1)
    await_bytes(x_rs.at[0], bytes_of(nt - 1, rows, feat))

    def up_second(off, carry):
        prepare(1, tensor_at(off))
        up_block(1, tensor_at(off))
        return carry

    lax.fori_loop(1, nt, up_second, 0)
    send_sums(1)
    send_up(1)
    if hi > 3:
        ring_step(0, 3)
    z_until(3, 2)
    finish_up(1)
    ring_step(1, 0)
    ring_step(0, hi)
    await_bytes(cs_rs.at[0], bytes_of(nt - 1, nz * part_rows, slice_width))

    def grad_some(first, last):
        @pl.when(core == 0)
        def _():
            if first == 0:
                grad_block(z, first=True)

            def one(i, carry):
                grad_block(plane_at(i))
                return carry

            lax.fori_loop(max(first, 1), last, one, 0)

    z_until(3, 3)
    grad_some(0, nz // 2)
    z_until(3, hi)
    ring_step(1, 1)
    hidden_landing(1).wait_recv()
    down1 = functools.partial(down_block, 1)
    down_block(1, z)
    for d in range(1, lo + 1):
        use_near(3, d, down1)
    use_far(3, down1)
    grad_some(nz // 2, nz)

    @pl.when(core == 0)
    def _():
        gsend[...] = gacc[0].astype(BF16)
        grad_copy().start()

    def grad_step(d):
        if d == 0:
            grad_block(z, first=True)
        elif d <= lo:

            def both(i, carry):
                grad_block(plane_at(d - 2 * d * i))
                return carry

            lax.fori_loop(0, 2, both, 0)
        else:
            grad_block(plane_at(d))

    middle = max(1, hi // 2)

    @pl.when(core == 1)
    def _():
        for d in range(middle + 1):
            if d > 1:
                ring_step(1, d)
            grad_step(d)

    finish_down(1)

    @pl.when(core == 1)
    def _():
        for d in range(middle + 1, hi + 1):
            ring_step(1, d)
            grad_step(d)
        gsend[...] = gacc[0].astype(BF16)
        grad_copy().start()

    await_bytes(st_rs.at[0], bytes_of(3, h2, feat))
    state_store = pltpu.make_async_copy(state_buf, state_out, end_sem.at[0])
    state_store.start()
    grad_copy().wait_recv()
    grad_copy().wait_send()
    gsend[...] = (gacc[1] + grecv[...].astype(F32)).astype(BF16)
    grad_store = pltpu.make_async_copy(gsend, grad_out, end_sem.at[1])
    grad_store.start()

    block_bytes = bytes_of(feat, hidden)
    passed = 2 * sections * (2 * lo + 1) * block_bytes // 2
    await_bytes(hops, passed)
    await_bytes(pushes, passed + 2 * block_bytes)
    await_gains(gain_sends)
    await_bytes(
        others,
        bytes_of(2 * nt - 1, h2, feat)
        + bytes_of(nz - 1, part_rows, slice_width)
        + bytes_of(nt - 1, nz * part_rows, slice_width)
        + sections * bytes_of(h2, LANES, size=4)
        + (2 * sections + 1 + 2 * (nz - 1)) * bytes_of(h2, hidden)
        + (sections + 1) * bytes_of(nt - 1, rows, feat)
        + 3 * bytes_of(h2, feat),
    )
    state_store.wait()
    grad_store.wait()


def stack(sizes, tokens, gain, w_up, w_down, cotangent):
    sections, dp_count, nt = sizes
    nz = dp_count // INNER
    assert sections == 2 and nz == nt and nz % 2 == 0
    rows, slice_width = tokens.shape
    feat = slice_width // INNER
    h2 = rows // sections
    hidden = w_up.shape[2]
    assert w_up.shape[1] == feat and w_down.shape[2] == feat
    width = slice_width * nt
    hi = nz // 2
    dma = pltpu.SemaphoreType.DMA
    hbm = pl.BlockSpec(memory_space=pl.ANY)
    vmem = pl.BlockSpec(memory_space=pltpu.VMEM)

    def buf(*dims, dtype=BF16):
        return pltpu.VMEM(dims, dtype)

    return pl.pallas_call(
        functools.partial(stack_kernel, sizes, width),
        name="stack",
        out_shape=(
            jax.ShapeDtypeStruct((rows, slice_width), BF16),
            jax.ShapeDtypeStruct((hidden, feat), BF16),
        ),
        in_specs=[hbm, vmem, hbm, hbm, hbm],
        out_specs=(hbm, hbm),
        scratch_shapes=[
            buf(rows, slice_width),
            buf(1, slice_width, dtype=F32),
            buf(sections * nt, 1, feat, dtype=F32),
            buf(sections, nz, feat, hidden),
            buf(sections * nz * hidden, feat),
            buf(sections + 1, nt, rows, feat),
            buf(nt, rows, feat),
            buf(rows, LANES, dtype=F32),
            buf(rows, hidden, dtype=F32),
            buf(sections, h2, LANES, dtype=F32),
            buf(sections, h2, LANES, dtype=F32),
            buf(sections, h2, hidden),
            buf(sections, h2, hidden),
            buf(sections, rows, hidden),
            buf(sections, nt, rows, feat),
            buf(sections, nt, rows, feat),
            buf(rows, slice_width),
            buf(nz, rows, hidden),
            buf(nz, rows, slice_width),
            buf(2, hidden, feat, dtype=F32),
            buf(hidden, feat),
            buf(hidden, feat),
            dma((5,)),
            dma((1,)),
            dma((1,)),
            dma((1,)),
            dma((2 * sections, PIECES, hi)),
            dma((2 * sections, hi + 1)),
            dma((1,)),
            dma((1,)),
            dma((sections,)),
            dma((sections,)),
            dma((sections,)),
            dma((sections,)),
            dma((2, 2, hi)),
            dma((sections,)),
            dma((1,)),
            dma((1,)),
            dma((1,)),
            dma((2,)),
        ],
        compiler_params=pltpu.CompilerParams(collective_id=0, has_side_effects=True),
    )(tokens, gain, w_up, w_down, cotangent)


def body(tokens, gain, w_up, w_down, cotangent):
    sizes = (lax.axis_size("section"), lax.axis_size("dp"), lax.axis_size("tensor"))
    state, grad = stack(sizes, tokens, gain, w_up, w_down, cotangent)
    return (state[None], grad[None])


def solution(mesh):
    placed = (
        P("dp", "tensor"),
        P("section", "tensor"),
        P("section", "dp", "tensor"),
        P("section", "tensor", "dp"),
        P("section", "dp", None),
    )
    return jax.shard_map(
        body,
        mesh=mesh,
        in_specs=placed,
        out_specs=(P("section", "dp", "tensor"), P("section", "tensor", "dp")),
        check_vma=False,
    )
```

```python
import functools
import itertools

import jax
import jax.numpy as jnp
from jax import lax
from jax.experimental import pallas as pl
from jax.experimental.pallas import tpu as pltpu
from jax.sharding import PartitionSpec as P

EPS = 1e-06
F32 = jnp.float32
BF16 = jnp.bfloat16

MESH = pl.DeviceIdType.MESH
LANES = 128
PIECES = 8
INNER = 2
RING_PARTS = 2
VMEM_BYTES = 40 * 1024 * 1024


def far_first(count):
    return sorted(range(1, count), key=lambda k: abs(2 * k - count))


def remote(src, dst, send_sem, recv_sem, target):
    return pltpu.make_async_remote_copy(
        src_ref=src,
        dst_ref=dst,
        send_sem=send_sem,
        recv_sem=recv_sem,
        device_id=target,
        device_id_type=MESH,
    )


def stack_kernel(
    sizes,
    width,
    tok_ref,
    gain_ref,
    up_ref,
    down_ref,
    cot_ref,
    state_buf,
    near_out,
    grecv,
    tok,
    gain_f,
    gains,
    wu,
    wd,
    xb,
    xg,
    ssq,
    acc,
    sq_send,
    sq_recv,
    up_send,
    up_recv,
    hid,
    part_send,
    part_recv,
    hg,
    cb,
    gacc,
    gsend,
    send_sem,
    load_sem,
    tk_rs,
    ga_rs,
    z_rs,
    f_rs,
    c_rs,
    cs_rs,
    sq_rs,
    ux_rs,
    ax_rs,
    hd_rs,
    h_rs,
    p_rs,
    x_rs,
    st_rs,
    gx_rs,
):
    sections, dp_count, nt = sizes
    nz = dp_count // INNER
    hi = nz // 2
    lo = nz - 1 - hi
    rows, slice_width = tok.shape
    h2 = rows // sections
    feat = slice_width // INNER
    part_rows = rows // nt
    hidden = wu.shape[3]

    core = lax.axis_index("section")
    t = lax.axis_index("tensor")
    me = lax.axis_index("dp")
    z = me // INNER
    q = lax.rem(me, INNER)
    other = 1 - core
    sign = 1 - 2 * core
    beside = z * INNER + 1 - q

    def block_of(index, size):
        if isinstance(index, int):
            return pl.ds(index * size, size)
        return pl.ds(pl.multiple_of(index * size, size), size)

    mine = block_of(q, h2)
    theirs = block_of(1 - q, h2)
    core_rows = block_of(core, h2)
    other_rows = block_of(other, h2)
    my_cols = block_of(q, feat)
    their_cols = block_of(1 - q, feat)
    my_part = block_of(t, part_rows)

    hops, pushes, others, gain_sends, grad_sends = (send_sem.at[i] for i in range(5))

    def bytes_of(*dims, size=2):
        count = size
        for dim in dims:
            count *= dim
        return count

    def await_bytes(sem, count):
        ref = wd.at[pl.ds(0, count // (2 * feat))]
        pltpu.make_async_copy(ref, ref, sem).wait()

    def down_rows(layer, origin, piece=0, pieces=1):
        return block_of((layer * nz + origin) * pieces + piece, hidden // pieces)

    def tensor_at(off):
        return lax.rem(t + off, nt)

    def plane_at(shift):
        return lax.rem(z + nz + shift, nz)

    def launch(make, *args, cond=None):
        if cond is None:
            make(*args).start()
        else:
            pl.when(cond())(lambda: make(*args).start())

    loads = [
        pltpu.make_async_copy(up_ref.at[0], wu.at[core, z], load_sem.at[0]),
        pltpu.make_async_copy(tok_ref, tok, load_sem.at[0]),
        pltpu.make_async_copy(down_ref.at[0], wd.at[down_rows(core, z)], load_sem.at[0]),
        pltpu.make_async_copy(
            cot_ref.at[0, my_part, block_of(z, slice_width)], cb.at[z, my_part], load_sem.at[0]
        ),
    ]
    for copy in loads:
        copy.start()

    barrier = pltpu.get_barrier_semaphore()

    def greet(target):
        pl.semaphore_signal(barrier, inc=1, device_id=target, device_id_type=MESH)

    for m in far_first(nz):
        greet({"dp": plane_at(m) * INNER + q})
    for off in far_first(nt) + [0]:
        greet({"dp": beside, "tensor": tensor_at(off)})
        greet({"section": other, "tensor": tensor_at(off)})
        if off:
            greet({"tensor": tensor_at(off)})
    greet({"section": other, "dp": beside})

    gain_f[...] = gain_ref[...].astype(F32)
    gains[core * nt + t] = gain_f[:, my_cols]
    ssq[...] = jnp.zeros_like(ssq)
    await_bytes(
        load_sem.at[0],
        bytes_of(2, feat, hidden) + bytes_of(rows, slice_width) + bytes_of(part_rows, slice_width),
    )
    xb[0, t, mine] = tok[core_rows, my_cols]

    pl.semaphore_wait(barrier, (nz - 1) + (2 * nt - 1) + nt + 1)

    def weight(layer, kind, origin, piece, pieces=PIECES):
        if kind:
            return wd.at[down_rows(layer, origin, piece, pieces)]
        return wu.at[layer, origin, block_of(piece, feat // pieces)]

    def along(d):
        return plane_at(-sign * d)

    def against(d):
        return plane_at(sign * d)

    def hop(m, piece, s):
        ref = weight(m // 2, m % 2, along(s), piece)
        return remote(
            ref,
            ref,
            hops,
            z_rs.at[m, piece, s],
            {"dp": plane_at(sign) * INNER + q},
        )

    def landing(m, piece, d):
        ref = weight(m // 2, m % 2, along(d), piece)
        return remote(
            ref,
            ref,
            hops,
            z_rs.at[m, piece, d - 1],
            {"dp": plane_at(sign) * INNER + q},
        )

    def push(m, piece, d):
        ref = weight(m // 2, m % 2, along(d), piece)
        return remote(
            ref, ref, pushes, f_rs.at[m, d], {"section": other}
        )

    def pushed(m, d):
        ref = weight(m // 2, m % 2, against(d), 0, 2 if d == hi else 1)
        return remote(ref, ref, pushes, f_rs.at[m, d], {"section": other})

    def push_own(kind, piece):
        ref = weight(core, kind, z, piece)
        m = 2 * core + kind
        return remote(
            ref, ref, pushes, f_rs.at[m, 0], {"section": other}
        )

    def lacks(layer):
        return lambda: core != layer

    half = PIECES // 2
    far_pieces = [core * half + j for j in range(half)]
    near_pieces = [other * half + j for j in range(half)]

    def begin(m):
        @pl.when(core != m // 2)
        def _():
            pushed(m, 0).wait_recv()

        for piece in range(PIECES) if lo else far_pieces:
            launch(hop, m, piece, 0)

    def advance(m, d):
        for piece in range(PIECES) if d < lo else far_pieces:
            landing(m, piece, d).wait_recv()
            if d < hi:
                launch(hop, m, piece, d)
            launch(push, m, piece, d)
        if d == max(lo, 1) and m + 1 < 2 * sections:
            begin(m + 1)
        if d == lo:
            for piece in near_pieces:
                landing(m, piece, d).wait_recv()
                launch(push, m, piece, d)

    rounds = [(m, d) for m in range(2 * sections) for d in range(1, hi + 1)]
    done_rounds = [0]

    def z_until(m, d):
        last = rounds.index((m, min(d, hi))) + 1
        for r in range(done_rounds[0], last):
            advance(*rounds[r])
        done_rounds[0] = max(done_rounds[0], last)

    def take(m, d):
        pushed(m, d).wait_recv()

    def take_far(m):
        pushed(m, hi).wait_recv()

    for piece in range(PIECES):
        launch(push_own, 0, piece)

    @pl.when(core == 0)
    def _():
        for piece in range(PIECES) if lo else far_pieces:
            hop(0, piece, 0).start()

    def token_copy(away, off):
        cols, dp = (their_cols, beside) if away else (my_cols, me)
        return remote(
            tok.at[core_rows, cols],
            xb.at[0, t, mine],
            others,
            tk_rs.at[0],
            {"dp": dp, "tensor": tensor_at(off)},
        )

    for off in far_first(nt) + [0]:
        launch(token_copy, 1, off)
        if off:
            launch(token_copy, 0, off)

    def gain_copy(away, off):
        return remote(
            gains.at[core * nt + t],
            gains.at[core * nt + t],
            gain_sends,
            ga_rs.at[0],
            {"section": other if away else core, "tensor": tensor_at(off)},
        )

    def await_gains(sem):
        ref = gains.at[pl.ds(0, sections * nt - 1)]
        pltpu.make_async_copy(ref, ref, sem).wait()

    for off in far_first(nt) + [0]:
        launch(gain_copy, 1, off)
        if off:
            launch(gain_copy, 0, off)
    for piece in range(PIECES):
        launch(push_own, 1, piece)

    def cot_copy(m):
        to = plane_at(m)
        return remote(
            cot_ref.at[0, my_part, block_of(to, slice_width)],
            cb.at[z, my_part],
            others,
            c_rs.at[0],
            {"dp": to * INNER + q},
        )

    @pl.when(core != 0)
    def _():
        pushed(0, 0).wait_recv()
        for piece in range(PIECES) if lo else far_pieces:
            hop(0, piece, 0).start()

    for m in far_first(nz):
        launch(cot_copy, m)

    def cot_share(off):
        ref = cb.at[:, my_part]
        return remote(ref, ref, others, cs_rs.at[0], {"tensor": tensor_at(off)})

    def await_cotangent():
        await_bytes(c_rs.at[0], bytes_of(nz - 1, part_rows, slice_width))

    def share_cotangent(first, last):
        for off in far_first(nt)[first:last]:
            launch(cot_share, off)

    def prepare(layer, block):
        x = xb[layer, block].astype(F32)
        xg[block] = (x * gains[layer * nt + block]).astype(BF16)
        square = x * x
        total = ssq[...]
        for lower in range(0, feat, LANES):
            total = total + square[:, lower : lower + LANES]
        ssq[...] = total

    def up_block(layer, block, first=False):
        value = jnp.dot(xg[block], wu[layer, block], preferred_element_type=F32)
        acc[...] = value if first else acc[...] + value

    def sum_copy(layer):
        return remote(
            sq_send.at[layer], sq_recv.at[layer], others, sq_rs.at[layer], {"dp": beside}
        )

    def send_sums(layer):
        sq_send[layer] = jnp.broadcast_to(
            jnp.sum(ssq[theirs], axis=1, keepdims=True), (h2, LANES)
        )
        launch(sum_copy, layer)

    def up_copy(layer):
        return remote(
            up_send.at[layer], up_recv.at[layer], others, ux_rs.at[layer], {"dp": beside}
        )

    def send_up(layer):
        up_send[layer] = acc[theirs].astype(BF16)
        launch(up_copy, layer)

    def hidden_copy(layer):
        ref = hid.at[layer, mine]
        return remote(ref, ref, others, ax_rs.at[layer], {"dp": beside})

    def hidden_landing(layer):
        ref = hid.at[layer, theirs]
        return remote(ref, ref, others, ax_rs.at[layer], {"dp": beside})

    def hidden_give(layer):
        return remote(
            hid.at[layer, mine],
            hg.at[z, core_rows],
            others,
            hd_rs.at[layer],
            {"section": other},
        )

    def hidden_given(layer):
        ref = hg.at[z, other_rows]
        return remote(ref, ref, others, hd_rs.at[layer], {"section": other})

    def finish_up(layer):
        sum_copy(layer).wait_recv()
        total = jnp.sum(ssq[mine], axis=1, keepdims=True) + sq_recv[layer]
        inverse = lax.rsqrt(total / width + EPS)
        up_copy(layer).wait_recv()
        for lower in range(0, hidden, LANES):
            cols = pl.ds(lower, LANES)
            value = (acc[mine, cols] + up_recv[layer, :, cols].astype(F32)) * inverse
            hid[layer, mine, cols] = jax.nn.gelu(value, approximate=True).astype(BF16)
        launch(hidden_copy, layer)
        launch(hidden_give, layer, cond=lacks(layer))

        @pl.when(core == layer)
        def _():
            hg[z, core_rows] = hid[layer, mine]

        if layer == 0:
            ssq[...] = jnp.zeros_like(ssq)

    def ring_length(k, way):
        return hi if k == way else lo

    def ring_ref(k, part, origin, layer):
        whose = layer if k == 0 else 1 - layer
        return hg.at[origin, block_of(whose * RING_PARTS + part, h2 // RING_PARTS)]

    def ring_copy(k, part, way, s, layer):
        delta = 1 if way == 0 else -1
        ref = ring_ref(k, part, plane_at(-delta * s), layer)
        return remote(
            ref,
            ref,
            others,
            h_rs.at[k * RING_PARTS + part, way, s],
            {"dp": plane_at(delta) * INNER + q},
        )

    def ring_landing(k, part, way, d, layer):
        delta = 1 if way == 0 else -1
        ref = ring_ref(k, part, plane_at(-delta * d), layer)
        return remote(
            ref,
            ref,
            others,
            h_rs.at[k * RING_PARTS + part, way, d - 1],
            {"dp": plane_at(delta) * INNER + q},
        )

    def ring_step(layer, d):
        @pl.when(core == layer)
        def _():
            for k in range(2):
                if d == 0 and k == 1:
                    hidden_given(layer).wait_recv()
                for part, way in itertools.product(range(RING_PARTS), range(2)):
                    length = ring_length(k, way)
                    if 0 < d <= length:
                        ring_landing(k, part, way, d, layer).wait_recv()
                    if d < length:
                        ring_copy(k, part, way, d, layer).start()

    def part_copy(layer, block):
        return remote(
            part_send.at[layer, block],
            part_recv.at[layer, t],
            others,
            p_rs.at[layer],
            {"tensor": block},
        )

    def down_block(layer, block):
        part_send[layer, block] = jnp.dot(
            hid[layer], wd[down_rows(layer, block)], preferred_element_type=F32
        ).astype(BF16)

        @pl.when(block != t)
        def _():
            part_copy(layer, block).start()

    def next_copy(off):
        ref = xb.at[1, t]
        return remote(ref, ref, others, x_rs.at[0], {"tensor": tensor_at(off)})

    def state_copy(layer, away):
        return remote(
            xb.at[layer + 1, t, theirs if away else mine],
            state_buf.at[core_rows, my_cols],
            others,
            st_rs.at[0],
            {"section": layer, "dp": beside} if away else {"section": other},
        )

    def finish_down(layer):
        value = xb[layer, t].astype(F32) + part_send[layer, t].astype(F32)
        await_bytes(p_rs.at[layer], bytes_of(nt - 1, rows, feat))
        for off in range(1, nt):
            value = value + part_recv[layer, tensor_at(off)].astype(F32)
        xb[layer + 1, t] = value.astype(BF16)
        if layer == 0:
            for off in far_first(nt):
                launch(next_copy, off)
        launch(state_copy, layer, 1)
        launch(state_copy, layer, 0, cond=lacks(layer))

        @pl.when(core == layer)
        def _():
            state_buf[core_rows, my_cols] = xb[layer + 1, t, mine]

    def grad_block(origin, first=False):
        left = hg[origin]
        for index, cols in ((0, their_cols), (1, my_cols)):
            value = lax.dot_general(
                left, cb[origin, :, cols], (((0,), (0,)), ((), ())), preferred_element_type=F32
            )
            total = near_out if index else gacc
            total[...] = value if first else total[...] + value

    def grad_copy():
        return remote(gsend, grecv, grad_sends, gx_rs.at[0], {"dp": beside})

    def give_grad():
        gsend[...] = gacc[...].astype(BF16)
        grad_copy().start()

    z_until(0, 2)
    await_bytes(tk_rs.at[0], bytes_of(2 * nt - 1, h2, feat))
    await_gains(ga_rs.at[0])

    def prepare_first(block, carry):
        prepare(0, block)
        return carry

    lax.fori_loop(0, nt, prepare_first, 0)
    send_sums(0)

    def use_near(m, d, use):
        use(along(d))
        take(m, d)
        use(against(d))

    def use_far(m, use):
        take_far(m)
        use(along(hi))

    up0 = functools.partial(up_block, 0)
    up_block(0, z, first=True)
    for d in range(1, lo + 1):
        z_until(0, d + 1)
        use_near(0, d, up0)
    z_until(0, hi)
    use_far(0, up0)
    send_up(0)
    await_cotangent()
    z_until(1, 1)
    finish_up(0)
    share_cotangent(0, nt // 2 - 1)
    z_until(1, hi)
    ring_step(0, 0)
    down0 = functools.partial(down_block, 0)
    hidden_landing(0).wait_recv()
    down_block(0, z)
    for d in range(1, lo + 1):
        use_near(1, d, down0)
    use_far(1, down0)
    z_until(2, 1)
    if hi > 1:
        ring_step(0, 1)
    z_until(2, 2)
    finish_down(0)
    share_cotangent(nt // 2 - 1, nt)
    if hi > 2:
        ring_step(0, 2)
    z_until(2, hi)

    prepare(1, t)
    for d in range(1, lo + 1):
        take(2, d)
    take_far(2)
    up_block(1, t, first=True)
    z_until(3, 1)
    await_bytes(x_rs.at[0], bytes_of(nt - 1, rows, feat))

    def up_second(off, carry):
        prepare(1, tensor_at(off))
        up_block(1, tensor_at(off))
        return carry

    lax.fori_loop(1, nt, up_second, 0)
    send_sums(1)
    send_up(1)
    if hi > 3:
        ring_step(0, 3)
    z_until(3, 2)
    finish_up(1)
    ring_step(1, 0)
    ring_step(0, hi)
    await_bytes(cs_rs.at[0], bytes_of(nt - 1, nz * part_rows, slice_width))

    def grad_some(first, last):
        @pl.when(core == 0)
        def _():
            if first == 0:
                grad_block(z, first=True)

            def one(i, carry):
                grad_block(plane_at(i))
                return carry

            lax.fori_loop(max(first, 1), last, one, 0)

    grad_some(0, nz)
    pl.when(core == 0)(lambda: give_grad())
    z_until(3, 3)
    if hi > 1:
        ring_step(1, 1)
    z_until(3, hi)
    hidden_landing(1).wait_recv()
    down1 = functools.partial(down_block, 1)
    down_block(1, z)
    for d in range(1, lo + 1):
        if d == lo and hi > 2:
            ring_step(1, 2)
        use_near(3, d, down1)
    use_far(3, down1)

    def grad_step(d):
        if d == 0:
            grad_block(z, first=True)
        elif d <= lo:

            def both(i, carry):
                grad_block(plane_at(d - 2 * d * i))
                return carry

            lax.fori_loop(0, 2, both, 0)
        else:
            grad_block(plane_at(d))

    ring_done = [2 if hi > 2 else 1 if hi > 1 else 0]

    def ring_and_grad(first, last):
        @pl.when(core == 1)
        def _():
            for d in range(first, last):
                if d > ring_done[0]:
                    ring_step(1, d)
                grad_step(d)

    ring_and_grad(0, hi)
    finish_down(1)

    ring_and_grad(hi, hi + 1)

    pl.when(core == 1)(lambda: give_grad())

    await_bytes(st_rs.at[0], bytes_of(3, h2, feat))
    grad_copy().wait_recv()
    grad_copy().wait_send()

    block_bytes = bytes_of(feat, hidden)
    passed = 2 * sections * (2 * lo + 1) * block_bytes // 2
    await_bytes(hops, passed)
    await_bytes(pushes, passed + 2 * block_bytes)
    await_gains(gain_sends)
    await_bytes(
        others,
        bytes_of(2 * nt - 1, h2, feat)
        + bytes_of(nz - 1, part_rows, slice_width)
        + bytes_of(nt - 1, nz * part_rows, slice_width)
        + sections * bytes_of(h2, LANES, size=4)
        + (2 * sections + 1 + 2 * (nz - 1)) * bytes_of(h2, hidden)
        + (sections + 1) * bytes_of(nt - 1, rows, feat)
        + 3 * bytes_of(h2, feat),
    )


def stack(sizes, tokens, gain, w_up, w_down, cotangent):
    sections, dp_count, nt = sizes
    nz = dp_count // INNER
    assert sections == 2 and nz == nt and nz % 2 == 0
    rows, slice_width = tokens.shape
    feat = slice_width // INNER
    h2 = rows // sections
    hidden = w_up.shape[2]
    assert w_up.shape[1] == feat and w_down.shape[2] == feat
    width = slice_width * nt
    hi = nz // 2
    dma = pltpu.SemaphoreType.DMA
    hbm = pl.BlockSpec(memory_space=pl.ANY)
    vmem = pl.BlockSpec(memory_space=pltpu.VMEM)

    def buf(*dims, dtype=BF16):
        return pltpu.VMEM(dims, dtype)

    return pl.pallas_call(
        functools.partial(stack_kernel, sizes, width),
        name="stack",
        out_shape=(
            jax.ShapeDtypeStruct((rows, slice_width), BF16),
            jax.ShapeDtypeStruct((hidden, feat), F32),
            jax.ShapeDtypeStruct((hidden, feat), BF16),
        ),
        in_specs=[hbm, vmem, hbm, hbm, hbm],
        out_specs=(vmem, vmem, vmem),
        scratch_shapes=[
            buf(rows, slice_width),
            buf(1, slice_width, dtype=F32),
            buf(sections * nt, 1, feat, dtype=F32),
            buf(sections, nz, feat, hidden),
            buf(sections * nz * hidden, feat),
            buf(sections + 1, nt, rows, feat),
            buf(nt, rows, feat),
            buf(rows, LANES, dtype=F32),
            buf(rows, hidden, dtype=F32),
            buf(sections, h2, LANES, dtype=F32),
            buf(sections, h2, LANES, dtype=F32),
            buf(sections, h2, hidden),
            buf(sections, h2, hidden),
            buf(sections, rows, hidden),
            buf(sections, nt, rows, feat),
            buf(sections, nt, rows, feat),
            buf(nz, rows, hidden),
            buf(nz, rows, slice_width),
            buf(hidden, feat, dtype=F32),
            buf(hidden, feat),
            dma((5,)),
            dma((1,)),
            dma((1,)),
            dma((1,)),
            dma((2 * sections, PIECES, hi)),
            dma((2 * sections, hi + 1)),
            dma((1,)),
            dma((1,)),
            dma((sections,)),
            dma((sections,)),
            dma((sections,)),
            dma((sections,)),
            dma((2 * RING_PARTS, 2, hi)),
            dma((sections,)),
            dma((1,)),
            dma((1,)),
            dma((1,)),
        ],
        compiler_params=pltpu.CompilerParams(
            collective_id=0, has_side_effects=True, vmem_limit_bytes=VMEM_BYTES
        ),
    )(tokens, gain, w_up, w_down, cotangent)


def finish_kernel(state_ref, near_ref, far_ref, state_out, grad_out):
    state_out[0] = state_ref[...]
    grad_out[0] = (near_ref[...] + far_ref[...].astype(F32)).astype(BF16)


def finish(state, near, far):
    vmem = pl.BlockSpec(memory_space=pltpu.VMEM)
    return pl.pallas_call(
        finish_kernel,
        name="finish",
        out_shape=(
            jax.ShapeDtypeStruct((1, *state.shape), BF16),
            jax.ShapeDtypeStruct((1, *far.shape), BF16),
        ),
        in_specs=[vmem] * 3,
        out_specs=(vmem, vmem),
        compiler_params=pltpu.CompilerParams(vmem_limit_bytes=VMEM_BYTES // 4),
    )(state, near, far)


def body(tokens, gain, w_up, w_down, cotangent):
    sizes = (lax.axis_size("section"), lax.axis_size("dp"), lax.axis_size("tensor"))
    arrays = [
        pltpu.with_memory_space_constraint(array, pltpu.HBM)
        for array in (tokens, gain, w_up, w_down, cotangent)
    ]
    return finish(*stack(sizes, *arrays))


def solution(mesh):
    placed = (
        P("dp", "tensor"),
        P("section", "tensor"),
        P("section", "dp", "tensor"),
        P("section", "tensor", "dp"),
        P("section", "dp", None),
    )
    return jax.shard_map(
        body,
        mesh=mesh,
        in_specs=placed,
        out_specs=(P("section", "dp", "tensor"), P("section", "tensor", "dp")),
        check_vma=False,
    )
```

```python
import functools
import itertools

import jax
import jax.numpy as jnp
from jax import lax
from jax.experimental import pallas as pl
from jax.experimental.pallas import tpu as pltpu
from jax.sharding import PartitionSpec as P

EPS = 1e-06
F32 = jnp.float32
BF16 = jnp.bfloat16

MESH = pl.DeviceIdType.MESH
LANES = 128
PIECES = 4
INNER = 2
RING_PARTS = 2
VMEM_BYTES = 40 * 1024 * 1024


def far_first(count):
    return sorted(range(1, count), key=lambda k: abs(2 * k - count))


def remote(src, dst, send_sem, recv_sem, target):
    return pltpu.make_async_remote_copy(
        src_ref=src,
        dst_ref=dst,
        send_sem=send_sem,
        recv_sem=recv_sem,
        device_id=target,
        device_id_type=MESH,
    )


def stack_kernel(
    sizes,
    width,
    tok_ref,
    gain_ref,
    up_ref,
    down_ref,
    cot_ref,
    state_buf,
    near_out,
    grecv,
    tok,
    gain_raw,
    gain_f,
    gains,
    wu,
    wd,
    xb,
    xg,
    ssq,
    acc,
    sq_send,
    sq_recv,
    up_send,
    up_recv,
    hid,
    part_send,
    part_recv,
    hg,
    cb,
    gacc,
    gsend,
    send_sem,
    load_sem,
    tk_rs,
    ga_rs,
    z_rs,
    f_rs,
    c_rs,
    cs_rs,
    sq_rs,
    ux_rs,
    ax_rs,
    hd_rs,
    h_rs,
    p_rs,
    x_rs,
    st_rs,
    gx_rs,
):
    sections, dp_count, nt = sizes
    nz = dp_count // INNER
    hi = nz // 2
    lo = nz - 1 - hi
    rows, slice_width = tok.shape
    h2 = rows // sections
    feat = slice_width // INNER
    part_rows = rows // nt
    hidden = wu.shape[3]

    core = lax.axis_index("section")
    t = lax.axis_index("tensor")
    me = lax.axis_index("dp")
    z = me // INNER
    q = lax.rem(me, INNER)
    other = 1 - core
    sign = 1 - 2 * core
    beside = z * INNER + 1 - q

    def block_of(index, size):
        if isinstance(index, int):
            return pl.ds(index * size, size)
        return pl.ds(pl.multiple_of(index * size, size), size)

    mine = block_of(q, h2)
    theirs = block_of(1 - q, h2)
    core_rows = block_of(core, h2)
    other_rows = block_of(other, h2)
    my_cols = block_of(q, feat)
    their_cols = block_of(1 - q, feat)
    my_part = block_of(t, part_rows)

    hops, pushes, others, gain_sends, grad_sends = (send_sem.at[i] for i in range(5))

    def bytes_of(*dims, size=2):
        count = size
        for dim in dims:
            count *= dim
        return count

    def await_bytes(sem, count):
        ref = wd.at[pl.ds(0, count // (2 * feat))]
        pltpu.make_async_copy(ref, ref, sem).wait()

    def down_rows(layer, origin, piece=0, pieces=1):
        return block_of((layer * nz + origin) * pieces + piece, hidden // pieces)

    def tensor_at(off):
        return lax.rem(t + off, nt)

    def plane_at(shift):
        return lax.rem(z + nz + shift, nz)

    def launch(make, *args, cond=None):
        if cond is None:
            make(*args).start()
        else:
            pl.when(cond())(lambda: make(*args).start())

    loads = [
        pltpu.make_async_copy(up_ref.at[0], wu.at[core, z], load_sem.at[0]),
        pltpu.make_async_copy(tok_ref, tok, load_sem.at[0]),
        pltpu.make_async_copy(down_ref.at[0], wd.at[down_rows(core, z)], load_sem.at[0]),
        pltpu.make_async_copy(
            cot_ref.at[0, my_part, block_of(z, slice_width)], cb.at[z, my_part], load_sem.at[0]
        ),
    ]
    gain_load = pltpu.make_async_copy(gain_ref, gain_raw, load_sem.at[1])
    gain_load.start()
    for copy in loads:
        copy.start()

    barrier = pltpu.get_barrier_semaphore()

    def greet(target):
        pl.semaphore_signal(barrier, inc=1, device_id=target, device_id_type=MESH)

    for m in far_first(nz):
        greet({"dp": plane_at(m) * INNER + q})
    for off in far_first(nt) + [0]:
        greet({"dp": beside, "tensor": tensor_at(off)})
        greet({"section": other, "tensor": tensor_at(off)})
        if off:
            greet({"tensor": tensor_at(off)})
    greet({"section": other, "dp": beside})

    gain_load.wait()
    gain_f[...] = gain_raw[...].astype(F32)
    gains[core * nt + t] = gain_f[:, my_cols]
    ssq[...] = jnp.zeros_like(ssq)
    await_bytes(
        load_sem.at[0],
        bytes_of(2, feat, hidden) + bytes_of(rows, slice_width) + bytes_of(part_rows, slice_width),
    )
    xb[0, t, mine] = tok[core_rows, my_cols]

    pl.semaphore_wait(barrier, (nz - 1) + (2 * nt - 1) + nt + 1)

    def weight(layer, kind, origin, piece, pieces=PIECES):
        if kind:
            return wd.at[down_rows(layer, origin, piece, pieces)]
        return wu.at[layer, origin, block_of(piece, feat // pieces)]

    def along(d):
        return plane_at(-sign * d)

    def against(d):
        return plane_at(sign * d)

    def hop(m, piece, s):
        ref = weight(m // 2, m % 2, along(s), piece)
        return remote(
            ref,
            ref,
            hops,
            z_rs.at[m % 3, piece, s],
            {"dp": plane_at(sign) * INNER + q},
        )

    def landing(m, piece, d):
        ref = weight(m // 2, m % 2, along(d), piece)
        return remote(
            ref,
            ref,
            hops,
            z_rs.at[m % 3, piece, d - 1],
            {"dp": plane_at(sign) * INNER + q},
        )

    def push(m, piece, d):
        ref = weight(m // 2, m % 2, along(d), piece)
        return remote(
            ref, ref, pushes, f_rs.at[m, d], {"section": other}
        )

    def pushed(m, d):
        ref = weight(m // 2, m % 2, against(d), 0, 2 if d == hi else 1)
        return remote(ref, ref, pushes, f_rs.at[m, d], {"section": other})

    def push_own(kind, piece):
        ref = weight(core, kind, z, piece)
        m = 2 * core + kind
        return remote(
            ref, ref, pushes, f_rs.at[m, 0], {"section": other}
        )

    def lacks(layer):
        return lambda: core != layer

    half = PIECES // 2
    far_pieces = [core * half + j for j in range(half)]
    near_pieces = [other * half + j for j in range(half)]

    def begin(m):
        @pl.when(core != m // 2)
        def _():
            pushed(m, 0).wait_recv()

        for piece in range(PIECES) if lo else far_pieces:
            launch(hop, m, piece, 0)

    def advance(m, d, between=None):
        far = d >= lo
        for count, piece in enumerate(far_pieces if far else range(PIECES)):
            landing(m, piece, d).wait_recv()
            if d < hi:
                launch(hop, m, piece, d)
            launch(push, m, piece, d)
            if between is not None:
                between(count)
        if d == max(lo, 1) and m + 1 < 2 * sections:
            begin(m + 1)
        if d == lo:
            for count, piece in enumerate(near_pieces):
                landing(m, piece, d).wait_recv()
                launch(push, m, piece, d)
                if between is not None:
                    between(half + count)
        elif far and between is not None:
            for count in range(half, PIECES):
                between(count)

    rounds = [(m, d) for m in range(2 * sections) for d in range(1, hi + 1)]
    done_rounds = [0]

    def z_until(m, d, between=None):
        last = rounds.index((m, min(d, hi))) + 1
        for r in range(done_rounds[0], last):
            advance(*rounds[r], between if r == last - 1 else None)
        done_rounds[0] = max(done_rounds[0], last)

    def spread(count, do):
        def between(step):
            for i in range(step * count // PIECES, (step + 1) * count // PIECES):
                do(i)

        return between

    def take(m, d):
        pushed(m, d).wait_recv()

    def take_far(m):
        pushed(m, hi).wait_recv()

    for piece in range(PIECES):
        launch(push_own, 0, piece)

    @pl.when(core == 0)
    def _():
        for piece in range(PIECES) if lo else far_pieces:
            hop(0, piece, 0).start()

    def token_copy(away, off):
        cols, dp = (their_cols, beside) if away else (my_cols, me)
        return remote(
            tok.at[core_rows, cols],
            xb.at[0, t, mine],
            others,
            tk_rs.at[0],
            {"dp": dp, "tensor": tensor_at(off)},
        )

    for off in far_first(nt) + [0]:
        launch(token_copy, 1, off)
        if off:
            launch(token_copy, 0, off)

    def gain_copy(away, off):
        return remote(
            gains.at[core * nt + t],
            gains.at[core * nt + t],
            gain_sends,
            ga_rs.at[0],
            {"section": other if away else core, "tensor": tensor_at(off)},
        )

    def await_gains(sem):
        ref = gains.at[pl.ds(0, sections * nt - 1)]
        pltpu.make_async_copy(ref, ref, sem).wait()

    for off in far_first(nt) + [0]:
        launch(gain_copy, 1, off)
        if off:
            launch(gain_copy, 0, off)
    for piece in range(PIECES):
        launch(push_own, 1, piece)

    def cot_copy(m):
        to = plane_at(m)
        return remote(
            cot_ref.at[0, my_part, block_of(to, slice_width)],
            cb.at[z, my_part],
            others,
            c_rs.at[0],
            {"dp": to * INNER + q},
        )

    @pl.when(core != 0)
    def _():
        pushed(0, 0).wait_recv()
        for piece in range(PIECES) if lo else far_pieces:
            hop(0, piece, 0).start()

    for m in far_first(nz):
        launch(cot_copy, m)

    def cot_share(off):
        ref = cb.at[:, my_part]
        return remote(ref, ref, others, cs_rs.at[0], {"tensor": tensor_at(off)})

    def await_cotangent():
        await_bytes(c_rs.at[0], bytes_of(nz - 1, part_rows, slice_width))

    def share_cotangent(first, last):
        for off in far_first(nt)[first:last]:
            launch(cot_share, off)

    def prepare(layer, block):
        x = xb[layer, block].astype(F32)
        xg[block] = (x * gains[layer * nt + block]).astype(BF16)
        square = x * x
        total = ssq[...]
        for lower in range(0, feat, LANES):
            total = total + square[:, lower : lower + LANES]
        ssq[...] = total

    def up_block(layer, block, first=False):
        value = jnp.dot(xg[block], wu[layer, block], preferred_element_type=F32)
        acc[...] = value if first else acc[...] + value

    def sum_copy(layer):
        return remote(
            sq_send.at[layer], sq_recv.at[layer], others, sq_rs.at[layer], {"dp": beside}
        )

    def send_sums(layer):
        sq_send[layer] = jnp.broadcast_to(
            jnp.sum(ssq[theirs], axis=1, keepdims=True), (h2, LANES)
        )
        launch(sum_copy, layer)

    def up_copy(layer):
        return remote(
            up_send.at[layer], up_recv.at[layer], others, ux_rs.at[layer], {"dp": beside}
        )

    def send_up(layer):
        up_send[layer] = acc[theirs].astype(BF16)
        launch(up_copy, layer)

    def hidden_copy(layer):
        ref = hid.at[layer, mine]
        return remote(ref, ref, others, ax_rs.at[layer], {"dp": beside})

    def hidden_landing(layer):
        ref = hid.at[layer, theirs]
        return remote(ref, ref, others, ax_rs.at[layer], {"dp": beside})

    def hidden_give(layer):
        return remote(
            hid.at[layer, mine],
            hg.at[z, core_rows],
            others,
            hd_rs.at[layer],
            {"section": other},
        )

    def hidden_given(layer):
        ref = hg.at[z, other_rows]
        return remote(ref, ref, others, hd_rs.at[layer], {"section": other})

    def finish_up(layer):
        sum_copy(layer).wait_recv()
        total = jnp.sum(ssq[mine], axis=1, keepdims=True) + sq_recv[layer]
        inverse = lax.rsqrt(total / width + EPS)
        up_copy(layer).wait_recv()
        for lower in range(0, hidden, LANES):
            cols = pl.ds(lower, LANES)
            value = (acc[mine, cols] + up_recv[layer, :, cols].astype(F32)) * inverse
            hid[layer, mine, cols] = jax.nn.gelu(value, approximate=True).astype(BF16)
        launch(hidden_copy, layer)
        launch(hidden_give, layer, cond=lacks(layer))

        @pl.when(core == layer)
        def _():
            hg[z, core_rows] = hid[layer, mine]

        if layer == 0:
            ssq[...] = jnp.zeros_like(ssq)

    def ring_length(k, way):
        return hi if k == way else lo

    def ring_ref(k, part, origin, layer):
        whose = layer if k == 0 else 1 - layer
        return hg.at[origin, block_of(whose * RING_PARTS + part, h2 // RING_PARTS)]

    def ring_copy(k, part, way, s, layer):
        delta = 1 if way == 0 else -1
        ref = ring_ref(k, part, plane_at(-delta * s), layer)
        return remote(
            ref,
            ref,
            others,
            h_rs.at[k * RING_PARTS + part, way, s],
            {"dp": plane_at(delta) * INNER + q},
        )

    def ring_landing(k, part, way, d, layer):
        delta = 1 if way == 0 else -1
        ref = ring_ref(k, part, plane_at(-delta * d), layer)
        return remote(
            ref,
            ref,
            others,
            h_rs.at[k * RING_PARTS + part, way, d - 1],
            {"dp": plane_at(delta) * INNER + q},
        )

    def ring_step(layer, d):
        @pl.when(core == layer)
        def _():
            for k in range(2):
                if d == 0 and k == 1:
                    hidden_given(layer).wait_recv()
                for part, way in itertools.product(range(RING_PARTS), range(2)):
                    length = ring_length(k, way)
                    if 0 < d <= length:
                        ring_landing(k, part, way, d, layer).wait_recv()
                    if d < length:
                        ring_copy(k, part, way, d, layer).start()

    def part_copy(layer, block):
        return remote(
            part_send.at[layer, block],
            part_recv.at[layer, t],
            others,
            p_rs.at[layer],
            {"tensor": block},
        )

    def down_block(layer, block):
        part_send[layer, block] = jnp.dot(
            hid[layer], wd[down_rows(layer, block)], preferred_element_type=F32
        ).astype(BF16)

        @pl.when(block != t)
        def _():
            part_copy(layer, block).start()

    def next_copy(off):
        ref = xb.at[1, t]
        return remote(ref, ref, others, x_rs.at[0], {"tensor": tensor_at(off)})

    def state_copy(layer, away):
        return remote(
            xb.at[layer + 1, t, theirs if away else mine],
            state_buf.at[core_rows, my_cols],
            others,
            st_rs.at[0],
            {"section": layer, "dp": beside} if away else {"section": other},
        )

    def finish_down(layer):
        value = xb[layer, t].astype(F32) + part_send[layer, t].astype(F32)
        await_bytes(p_rs.at[layer], bytes_of(nt - 1, rows, feat))
        for off in range(1, nt):
            value = value + part_recv[layer, tensor_at(off)].astype(F32)
        xb[layer + 1, t] = value.astype(BF16)
        if layer == 0:
            for off in far_first(nt):
                launch(next_copy, off)
        launch(state_copy, layer, 1)
        launch(state_copy, layer, 0, cond=lacks(layer))

        @pl.when(core == layer)
        def _():
            state_buf[core_rows, my_cols] = xb[layer + 1, t, mine]

    def grad_block(origin, first=False, parts=(0, 1)):
        left = hg[origin]
        for index in parts:
            cols = my_cols if index else their_cols
            value = lax.dot_general(
                left, cb[origin, :, cols], (((0,), (0,)), ((), ())), preferred_element_type=F32
            )
            total = near_out if index else gacc
            total[...] = value if first else total[...] + value

    def grad_copy():
        return remote(gsend, grecv, grad_sends, gx_rs.at[0], {"dp": beside})

    def give_grad():
        gsend[...] = gacc[...].astype(BF16)
        grad_copy().start()

    z_until(0, 2)
    await_bytes(tk_rs.at[0], bytes_of(2 * nt - 1, h2, feat))
    await_gains(ga_rs.at[0])

    def prepare_first(block, carry):
        prepare(0, block)
        return carry

    lax.fori_loop(0, nt, prepare_first, 0)
    send_sums(0)

    def use_near(m, d, use):
        use(along(d))
        take(m, d)
        use(against(d))

    def use_far(m, use):
        take_far(m)
        use(along(hi))

    up0 = functools.partial(up_block, 0)
    up_block(0, z, first=True)
    for d in range(1, lo + 1):
        z_until(0, d + 1)
        use_near(0, d, up0)
    z_until(0, hi)
    use_far(0, up0)
    send_up(0)
    await_cotangent()
    z_until(1, 1)
    finish_up(0)
    share_cotangent(0, nt // 2 - 1)
    z_until(1, hi)
    ring_step(0, 0)
    down0 = functools.partial(down_block, 0)
    hidden_landing(0).wait_recv()
    down_block(0, z)
    for d in range(1, lo + 1):
        use_near(1, d, down0)
    use_far(1, down0)
    z_until(2, 1)
    if hi > 1:
        ring_step(0, 1)
    z_until(2, 2)
    finish_down(0)
    share_cotangent(nt // 2 - 1, nt)
    if hi > 2:
        ring_step(0, 2)
    z_until(2, hi)

    for d in range(1, lo + 1):
        take(2, d)
    take_far(2)
    await_bytes(x_rs.at[0], bytes_of(nt - 1, rows, feat))

    def up_second(off):
        prepare(1, tensor_at(off))
        up_block(1, tensor_at(off), first=off == 0)

    z_until(3, 1, spread(nt, up_second))
    send_sums(1)
    send_up(1)
    if hi > 3:
        ring_step(0, 3)
    z_until(3, 2)
    finish_up(1)
    ring_step(1, 0)
    ring_step(0, hi)
    await_bytes(cs_rs.at[0], bytes_of(nt - 1, nz * part_rows, slice_width))

    def grad_some(first, last):
        @pl.when(core == 0)
        def _():
            if first == 0:
                grad_block(z, first=True)

            def one(i, carry):
                grad_block(plane_at(i))
                return carry

            lax.fori_loop(max(first, 1), last, one, 0)

    grad_some(0, nz)
    pl.when(core == 0)(lambda: give_grad())
    z_until(3, 3)
    if hi > 1:
        ring_step(1, 1)
    z_until(3, hi)
    hidden_landing(1).wait_recv()
    down1 = functools.partial(down_block, 1)
    down_block(1, z)
    for d in range(1, lo + 1):
        if d == lo and hi > 2:
            ring_step(1, 2)
        use_near(3, d, down1)
    use_far(3, down1)

    def grad_step(d):
        if d == 0:
            grad_block(z, first=True)
        elif d <= lo:

            def both(i, carry):
                grad_block(plane_at(d - 2 * d * i))
                return carry

            lax.fori_loop(0, 2, both, 0)
        else:
            grad_block(plane_at(d))

    ring_done = [2 if hi > 2 else 1 if hi > 1 else 0]

    def ring_and_grad(first, last):
        @pl.when(core == 1)
        def _():
            for d in range(first, last):
                if d > ring_done[0]:
                    ring_step(1, d)
                grad_step(d)

    ring_and_grad(0, hi)
    finish_down(1)

    @pl.when(core == 1)
    def _():
        if hi > ring_done[0]:
            ring_step(1, hi)
        grad_block(plane_at(hi), parts=(0,))
        give_grad()
        grad_block(plane_at(hi), parts=(1,))


    await_bytes(st_rs.at[0], bytes_of(3, h2, feat))
    grad_copy().wait_recv()
    grad_copy().wait_send()

    block_bytes = bytes_of(feat, hidden)
    passed = 2 * sections * (2 * lo + 1) * block_bytes // 2
    await_bytes(hops, passed)
    await_bytes(pushes, passed + 2 * block_bytes)
    await_gains(gain_sends)
    await_bytes(
        others,
        bytes_of(2 * nt - 1, h2, feat)
        + bytes_of(nz - 1, part_rows, slice_width)
        + bytes_of(nt - 1, nz * part_rows, slice_width)
        + sections * bytes_of(h2, LANES, size=4)
        + (2 * sections + 1 + 2 * (nz - 1)) * bytes_of(h2, hidden)
        + (sections + 1) * bytes_of(nt - 1, rows, feat)
        + 3 * bytes_of(h2, feat),
    )


def stack(sizes, tokens, gain, w_up, w_down, cotangent):
    sections, dp_count, nt = sizes
    nz = dp_count // INNER
    assert sections == 2 and nz == nt and nz % 2 == 0
    rows, slice_width = tokens.shape
    feat = slice_width // INNER
    h2 = rows // sections
    hidden = w_up.shape[2]
    assert w_up.shape[1] == feat and w_down.shape[2] == feat
    width = slice_width * nt
    hi = nz // 2
    dma = pltpu.SemaphoreType.DMA
    hbm = pl.BlockSpec(memory_space=pl.ANY)
    vmem = pl.BlockSpec(memory_space=pltpu.VMEM)

    def buf(*dims, dtype=BF16):
        return pltpu.VMEM(dims, dtype)

    return pl.pallas_call(
        functools.partial(stack_kernel, sizes, width),
        name="stack",
        out_shape=(
            jax.ShapeDtypeStruct((rows, slice_width), BF16),
            jax.ShapeDtypeStruct((hidden, feat), F32),
            jax.ShapeDtypeStruct((hidden, feat), BF16),
        ),
        in_specs=[hbm] * 5,
        out_specs=(vmem, vmem, vmem),
        scratch_shapes=[
            buf(rows, slice_width),
            buf(1, slice_width),
            buf(1, slice_width, dtype=F32),
            buf(sections * nt, 1, feat, dtype=F32),
            buf(sections, nz, feat, hidden),
            buf(sections * nz * hidden, feat),
            buf(sections + 1, nt, rows, feat),
            buf(nt, rows, feat),
            buf(rows, LANES, dtype=F32),
            buf(rows, hidden, dtype=F32),
            buf(sections, h2, LANES, dtype=F32),
            buf(sections, h2, LANES, dtype=F32),
            buf(sections, h2, hidden),
            buf(sections, h2, hidden),
            buf(sections, rows, hidden),
            buf(sections, nt, rows, feat),
            buf(sections, nt, rows, feat),
            buf(nz, rows, hidden),
            buf(nz, rows, slice_width),
            buf(hidden, feat, dtype=F32),
            buf(hidden, feat),
            dma((5,)),
            dma((2,)),
            dma((1,)),
            dma((1,)),
            dma((3, PIECES, hi)),
            dma((2 * sections, hi + 1)),
            dma((1,)),
            dma((1,)),
            dma((sections,)),
            dma((sections,)),
            dma((sections,)),
            dma((sections,)),
            dma((2 * RING_PARTS, 2, hi)),
            dma((sections,)),
            dma((1,)),
            dma((1,)),
            dma((1,)),
        ],
        compiler_params=pltpu.CompilerParams(
            collective_id=0, has_side_effects=True, vmem_limit_bytes=VMEM_BYTES
        ),
    )(tokens, gain, w_up, w_down, cotangent)


def finish_kernel(state_ref, near_ref, far_ref, state_out, grad_out):
    state_out[0] = state_ref[...]
    grad_out[0] = (near_ref[...] + far_ref[...].astype(F32)).astype(BF16)


def finish(state, near, far):
    vmem = pl.BlockSpec(memory_space=pltpu.VMEM)
    return pl.pallas_call(
        finish_kernel,
        name="finish",
        out_shape=(
            jax.ShapeDtypeStruct((1, *state.shape), BF16),
            jax.ShapeDtypeStruct((1, *far.shape), BF16),
        ),
        in_specs=[vmem] * 3,
        out_specs=(vmem, vmem),
        compiler_params=pltpu.CompilerParams(vmem_limit_bytes=VMEM_BYTES // 4),
    )(state, near, far)


def body(tokens, gain, w_up, w_down, cotangent):
    sizes = (lax.axis_size("section"), lax.axis_size("dp"), lax.axis_size("tensor"))
    arrays = [
        pltpu.with_memory_space_constraint(array, pltpu.HBM)
        for array in (tokens, gain, w_up, w_down, cotangent)
    ]
    return finish(*stack(sizes, *arrays))


def solution(mesh):
    placed = (
        P("dp", "tensor"),
        P("section", "tensor"),
        P("section", "dp", "tensor"),
        P("section", "tensor", "dp"),
        P("section", "dp", None),
    )
    return jax.shard_map(
        body,
        mesh=mesh,
        in_specs=placed,
        out_specs=(P("section", "dp", "tensor"), P("section", "tensor", "dp")),
        check_vma=False,
    )
```

```python
import functools
import itertools

import jax
import jax.numpy as jnp
from jax import lax
from jax.experimental import pallas as pl
from jax.experimental.pallas import tpu as pltpu
from jax.sharding import PartitionSpec as P

EPS = 1e-06
F32 = jnp.float32
BF16 = jnp.bfloat16

MESH = pl.DeviceIdType.MESH
LANES = 128
PIECES = 8
INNER = 2
RING_PARTS = 2
VMEM_BYTES = 40 * 1024 * 1024


def far_first(count):
    return sorted(range(1, count), key=lambda k: abs(2 * k - count))


def remote(src, dst, send_sem, recv_sem, target):
    return pltpu.make_async_remote_copy(
        src_ref=src,
        dst_ref=dst,
        send_sem=send_sem,
        recv_sem=recv_sem,
        device_id=target,
        device_id_type=MESH,
    )


def stack_kernel(
    sizes,
    width,
    tok_ref,
    gain_ref,
    up_ref,
    down_ref,
    cot_ref,
    state_buf,
    near_out,
    grecv,
    tok,
    gain_raw,
    gain_f,
    gains,
    wu,
    wd,
    xb,
    xg,
    ssq,
    acc,
    sq_send,
    sq_recv,
    up_send,
    up_recv,
    hid,
    part_send,
    part_recv,
    hg,
    cb,
    gacc,
    gsend,
    send_sem,
    load_sem,
    tk_rs,
    ga_rs,
    z_rs,
    f_rs,
    c_rs,
    cs_rs,
    sq_rs,
    ux_rs,
    ax_rs,
    hd_rs,
    h_rs,
    p_rs,
    x_rs,
    st_rs,
    gx_rs,
):
    sections, dp_count, nt = sizes
    nz = dp_count // INNER
    hi = nz // 2
    lo = nz - 1 - hi
    rows, slice_width = tok.shape
    h2 = rows // sections
    feat = slice_width // INNER
    part_rows = rows // nt
    hidden = wu.shape[3]

    core = lax.axis_index("section")
    t = lax.axis_index("tensor")
    me = lax.axis_index("dp")
    z = me // INNER
    q = lax.rem(me, INNER)
    other = 1 - core
    sign = 1 - 2 * core
    beside = z * INNER + 1 - q

    def block_of(index, size):
        if isinstance(index, int):
            return pl.ds(index * size, size)
        return pl.ds(pl.multiple_of(index * size, size), size)

    mine = block_of(q, h2)
    theirs = block_of(1 - q, h2)
    core_rows = block_of(core, h2)
    other_rows = block_of(other, h2)
    my_cols = block_of(q, feat)
    their_cols = block_of(1 - q, feat)
    my_part = block_of(t, part_rows)

    hops, pushes, others, gain_sends, grad_sends = (send_sem.at[i] for i in range(5))

    def bytes_of(*dims, size=2):
        count = size
        for dim in dims:
            count *= dim
        return count

    def await_bytes(sem, count):
        ref = wd.at[pl.ds(0, count // (2 * feat))]
        pltpu.make_async_copy(ref, ref, sem).wait()

    def down_rows(layer, origin, piece=0, pieces=1):
        return block_of((layer * nz + origin) * pieces + piece, hidden // pieces)

    def tensor_at(off):
        return lax.rem(t + off, nt)

    def plane_at(shift):
        return lax.rem(z + nz + shift, nz)

    def launch(make, *args, cond=None):
        if cond is None:
            make(*args).start()
        else:
            pl.when(cond())(lambda: make(*args).start())

    loads = [
        pltpu.make_async_copy(up_ref.at[0], wu.at[core, z], load_sem.at[0]),
        pltpu.make_async_copy(tok_ref, tok, load_sem.at[0]),
        pltpu.make_async_copy(down_ref.at[0], wd.at[down_rows(core, z)], load_sem.at[0]),
        pltpu.make_async_copy(
            cot_ref.at[0, my_part, block_of(z, slice_width)], cb.at[z, my_part], load_sem.at[0]
        ),
    ]
    gain_load = pltpu.make_async_copy(gain_ref, gain_raw, load_sem.at[1])
    gain_load.start()
    for copy in loads:
        copy.start()

    barrier = pltpu.get_barrier_semaphore()

    def greet(target):
        pl.semaphore_signal(barrier, inc=1, device_id=target, device_id_type=MESH)

    for m in far_first(nz):
        greet({"dp": plane_at(m) * INNER + q})
    for off in far_first(nt) + [0]:
        greet({"dp": beside, "tensor": tensor_at(off)})
        greet({"section": other, "tensor": tensor_at(off)})
        if off:
            greet({"tensor": tensor_at(off)})
    greet({"section": other, "dp": beside})

    gain_load.wait()
    gain_f[...] = gain_raw[...].astype(F32)
    gains[core * nt + t] = gain_f[:, my_cols]
    ssq[...] = jnp.zeros_like(ssq)
    await_bytes(
        load_sem.at[0],
        bytes_of(2, feat, hidden) + bytes_of(rows, slice_width) + bytes_of(part_rows, slice_width),
    )
    xb[0, t, mine] = tok[core_rows, my_cols]

    pl.semaphore_wait(barrier, (nz - 1) + (2 * nt - 1) + nt + 1)

    def weight(layer, kind, origin, piece, pieces=PIECES):
        if kind:
            return wd.at[down_rows(layer, origin, piece, pieces)]
        return wu.at[layer, origin, block_of(piece, feat // pieces)]

    def along(d):
        return plane_at(-sign * d)

    def against(d):
        return plane_at(sign * d)

    def hop(m, piece, s):
        ref = weight(m // 2, m % 2, along(s), piece)
        return remote(
            ref,
            ref,
            hops,
            z_rs.at[m % 3, piece, s],
            {"dp": plane_at(sign) * INNER + q},
        )

    def landing(m, piece, d):
        ref = weight(m // 2, m % 2, along(d), piece)
        return remote(
            ref,
            ref,
            hops,
            z_rs.at[m % 3, piece, d - 1],
            {"dp": plane_at(sign) * INNER + q},
        )

    def push(m, piece, d):
        ref = weight(m // 2, m % 2, along(d), piece)
        return remote(
            ref, ref, pushes, f_rs.at[m, d], {"section": other}
        )

    def pushed(m, d):
        ref = weight(m // 2, m % 2, against(d), 0, 2 if d == hi else 1)
        return remote(ref, ref, pushes, f_rs.at[m, d], {"section": other})

    def push_own(kind, piece):
        ref = weight(core, kind, z, piece)
        m = 2 * core + kind
        return remote(
            ref, ref, pushes, f_rs.at[m, 0], {"section": other}
        )

    def lacks(layer):
        return lambda: core != layer

    half = PIECES // 2
    far_pieces = [core * half + j for j in range(half)]
    near_pieces = [other * half + j for j in range(half)]

    def begin(m):
        @pl.when(core != m // 2)
        def _():
            pushed(m, 0).wait_recv()

        for piece in range(PIECES) if lo else far_pieces:
            launch(hop, m, piece, 0)

    def advance(m, d, between=None):
        far = d >= lo
        for count, piece in enumerate(far_pieces if far else range(PIECES)):
            landing(m, piece, d).wait_recv()
            if d < hi:
                launch(hop, m, piece, d)
            launch(push, m, piece, d)
            if between is not None:
                between(count)
        if d == max(lo, 1) and m + 1 < 2 * sections:
            begin(m + 1)
        if d == lo:
            for count, piece in enumerate(near_pieces):
                landing(m, piece, d).wait_recv()
                launch(push, m, piece, d)
                if between is not None:
                    between(half + count)
        elif far and between is not None:
            for count in range(half, PIECES):
                between(count)

    rounds = [(m, d) for m in range(2 * sections) for d in range(1, hi + 1)]
    done_rounds = [0]

    def z_until(m, d, between=None):
        last = rounds.index((m, min(d, hi))) + 1
        for r in range(done_rounds[0], last):
            advance(*rounds[r], between if r == last - 1 else None)
        done_rounds[0] = max(done_rounds[0], last)

    def spread(count, do):
        def between(step):
            for i in range(step * count // PIECES, (step + 1) * count // PIECES):
                do(i)

        return between

    def take(m, d):
        pushed(m, d).wait_recv()

    def take_far(m):
        pushed(m, hi).wait_recv()

    for piece in range(PIECES):
        launch(push_own, 0, piece)

    @pl.when(core == 0)
    def _():
        for piece in range(PIECES) if lo else far_pieces:
            hop(0, piece, 0).start()

    def token_copy(away, off):
        cols, dp = (their_cols, beside) if away else (my_cols, me)
        return remote(
            tok.at[core_rows, cols],
            xb.at[0, t, mine],
            others,
            tk_rs.at[0],
            {"dp": dp, "tensor": tensor_at(off)},
        )

    for off in far_first(nt) + [0]:
        launch(token_copy, 1, off)
        if off:
            launch(token_copy, 0, off)

    def gain_copy(away, off):
        return remote(
            gains.at[core * nt + t],
            gains.at[core * nt + t],
            gain_sends,
            ga_rs.at[0],
            {"section": other if away else core, "tensor": tensor_at(off)},
        )

    def await_gains(sem):
        ref = gains.at[pl.ds(0, sections * nt - 1)]
        pltpu.make_async_copy(ref, ref, sem).wait()

    for off in far_first(nt) + [0]:
        launch(gain_copy, 1, off)
        if off:
            launch(gain_copy, 0, off)
    for piece in range(PIECES):
        launch(push_own, 1, piece)

    def cot_copy(m):
        to = plane_at(m)
        return remote(
            cot_ref.at[0, my_part, block_of(to, slice_width)],
            cb.at[z, my_part],
            others,
            c_rs.at[0],
            {"dp": to * INNER + q},
        )

    @pl.when(core != 0)
    def _():
        pushed(0, 0).wait_recv()
        for piece in range(PIECES) if lo else far_pieces:
            hop(0, piece, 0).start()

    for m in far_first(nz):
        launch(cot_copy, m)

    def cot_share(off):
        ref = cb.at[:, my_part]
        return remote(ref, ref, others, cs_rs.at[0], {"tensor": tensor_at(off)})

    def await_cotangent():
        await_bytes(c_rs.at[0], bytes_of(nz - 1, part_rows, slice_width))

    def share_cotangent(first, last):
        for off in far_first(nt)[first:last]:
            launch(cot_share, off)

    def prepare(layer, block):
        x = xb[layer, block].astype(F32)
        xg[block] = (x * gains[layer * nt + block]).astype(BF16)
        square = x * x
        total = ssq[...]
        for lower in range(0, feat, LANES):
            total = total + square[:, lower : lower + LANES]
        ssq[...] = total

    def up_block(layer, block, first=False):
        value = jnp.dot(xg[block], wu[layer, block], preferred_element_type=F32)
        acc[...] = value if first else acc[...] + value

    def sum_copy(layer):
        return remote(
            sq_send.at[layer], sq_recv.at[layer], others, sq_rs.at[layer], {"dp": beside}
        )

    def send_sums(layer):
        sq_send[layer] = jnp.broadcast_to(
            jnp.sum(ssq[theirs], axis=1, keepdims=True), (h2, LANES)
        )
        launch(sum_copy, layer)

    def up_copy(layer):
        return remote(
            up_send.at[layer], up_recv.at[layer], others, ux_rs.at[layer], {"dp": beside}
        )

    def send_up(layer):
        up_send[layer] = acc[theirs].astype(BF16)
        launch(up_copy, layer)

    def hidden_copy(layer):
        ref = hid.at[layer, mine]
        return remote(ref, ref, others, ax_rs.at[layer], {"dp": beside})

    def hidden_landing(layer):
        ref = hid.at[layer, theirs]
        return remote(ref, ref, others, ax_rs.at[layer], {"dp": beside})

    def hidden_give(layer):
        return remote(
            hid.at[layer, mine],
            hg.at[z, core_rows],
            others,
            hd_rs.at[layer],
            {"section": other},
        )

    def hidden_given(layer):
        ref = hg.at[z, other_rows]
        return remote(ref, ref, others, hd_rs.at[layer], {"section": other})

    def finish_up(layer):
        sum_copy(layer).wait_recv()
        total = jnp.sum(ssq[mine], axis=1, keepdims=True) + sq_recv[layer]
        inverse = lax.rsqrt(total / width + EPS)
        up_copy(layer).wait_recv()
        for lower in range(0, hidden, LANES):
            cols = pl.ds(lower, LANES)
            value = (acc[mine, cols] + up_recv[layer, :, cols].astype(F32)) * inverse
            hid[layer, mine, cols] = jax.nn.gelu(value, approximate=True).astype(BF16)
        launch(hidden_copy, layer)
        launch(hidden_give, layer, cond=lacks(layer))

        @pl.when(core == layer)
        def _():
            hg[z, core_rows] = hid[layer, mine]

        if layer == 0:
            ssq[...] = jnp.zeros_like(ssq)

    def ring_length(k, way):
        return hi if k == way else lo

    def ring_ref(k, part, origin, layer):
        whose = layer if k == 0 else 1 - layer
        return hg.at[origin, block_of(whose * RING_PARTS + part, h2 // RING_PARTS)]

    def ring_copy(k, part, way, s, layer):
        delta = 1 if way == 0 else -1
        ref = ring_ref(k, part, plane_at(-delta * s), layer)
        return remote(
            ref,
            ref,
            others,
            h_rs.at[k * RING_PARTS + part, way, s],
            {"dp": plane_at(delta) * INNER + q},
        )

    def ring_landing(k, part, way, d, layer):
        delta = 1 if way == 0 else -1
        ref = ring_ref(k, part, plane_at(-delta * d), layer)
        return remote(
            ref,
            ref,
            others,
            h_rs.at[k * RING_PARTS + part, way, d - 1],
            {"dp": plane_at(delta) * INNER + q},
        )

    def ring_step(layer, d):
        @pl.when(core == layer)
        def _():
            for k in range(2):
                if d == 0 and k == 1:
                    hidden_given(layer).wait_recv()
                for part, way in itertools.product(range(RING_PARTS), range(2)):
                    length = ring_length(k, way)
                    if 0 < d <= length:
                        ring_landing(k, part, way, d, layer).wait_recv()
                    if d < length:
                        ring_copy(k, part, way, d, layer).start()

    def part_copy(layer, block):
        return remote(
            part_send.at[layer, block],
            part_recv.at[layer, t],
            others,
            p_rs.at[layer],
            {"tensor": block},
        )

    def down_block(layer, block):
        part_send[layer, block] = jnp.dot(
            hid[layer], wd[down_rows(layer, block)], preferred_element_type=F32
        ).astype(BF16)

        @pl.when(block != t)
        def _():
            part_copy(layer, block).start()

    def next_copy(off):
        ref = xb.at[1, t]
        return remote(ref, ref, others, x_rs.at[0], {"tensor": tensor_at(off)})

    def state_copy(layer, away):
        return remote(
            xb.at[layer + 1, t, theirs if away else mine],
            state_buf.at[core_rows, my_cols],
            others,
            st_rs.at[0],
            {"section": layer, "dp": beside} if away else {"section": other},
        )

    def finish_down(layer):
        value = xb[layer, t].astype(F32) + part_send[layer, t].astype(F32)
        await_bytes(p_rs.at[layer], bytes_of(nt - 1, rows, feat))
        for off in range(1, nt):
            value = value + part_recv[layer, tensor_at(off)].astype(F32)
        xb[layer + 1, t] = value.astype(BF16)
        if layer == 0:
            for off in far_first(nt):
                launch(next_copy, off)
        launch(state_copy, layer, 1)
        launch(state_copy, layer, 0, cond=lacks(layer))

        @pl.when(core == layer)
        def _():
            state_buf[core_rows, my_cols] = xb[layer + 1, t, mine]

    def grad_block(origin, first=False, parts=(0, 1)):
        left = hg[origin]
        for index in parts:
            cols = my_cols if index else their_cols
            value = lax.dot_general(
                left, cb[origin, :, cols], (((0,), (0,)), ((), ())), preferred_element_type=F32
            )
            total = near_out if index else gacc
            total[...] = value if first else total[...] + value

    def grad_copy():
        return remote(gsend, grecv, grad_sends, gx_rs.at[0], {"dp": beside})

    def give_grad():
        gsend[...] = gacc[...].astype(BF16)
        grad_copy().start()

    z_until(0, 2)
    await_bytes(tk_rs.at[0], bytes_of(2 * nt - 1, h2, feat))
    await_gains(ga_rs.at[0])

    def prepare_first(block, carry):
        prepare(0, block)
        return carry

    lax.fori_loop(0, nt, prepare_first, 0)
    send_sums(0)

    def use_near(m, d, use):
        use(along(d))
        take(m, d)
        use(against(d))

    def use_far(m, use):
        take_far(m)
        use(along(hi))

    up0 = functools.partial(up_block, 0)
    up_block(0, z, first=True)
    for d in range(1, lo + 1):
        z_until(0, d + 1)
        use_near(0, d, up0)
    z_until(0, hi)
    use_far(0, up0)
    send_up(0)
    await_cotangent()
    z_until(1, 1)
    finish_up(0)
    share_cotangent(0, nt // 2 - 1)
    z_until(1, hi)
    ring_step(0, 0)
    down0 = functools.partial(down_block, 0)
    hidden_landing(0).wait_recv()
    down_block(0, z)
    for d in range(1, lo + 1):
        use_near(1, d, down0)
    use_far(1, down0)
    z_until(2, 1)
    if hi > 1:
        ring_step(0, 1)
    z_until(2, 2)
    finish_down(0)
    share_cotangent(nt // 2 - 1, nt)
    if hi > 2:
        ring_step(0, 2)
    z_until(2, hi)

    for d in range(1, lo + 1):
        take(2, d)
    take_far(2)
    await_bytes(x_rs.at[0], bytes_of(nt - 1, rows, feat))

    def up_second(off):
        prepare(1, tensor_at(off))
        up_block(1, tensor_at(off), first=off == 0)

    z_until(3, 1, spread(nt, up_second))
    send_sums(1)
    send_up(1)
    if hi > 3:
        ring_step(0, 3)
    z_until(3, 2)
    finish_up(1)
    ring_step(1, 0)
    ring_step(0, hi)
    await_bytes(cs_rs.at[0], bytes_of(nt - 1, nz * part_rows, slice_width))

    def grad_some(first, last):
        @pl.when(core == 0)
        def _():
            if first == 0:
                grad_block(z, first=True)

            def one(i, carry):
                grad_block(plane_at(i))
                return carry

            lax.fori_loop(max(first, 1), last, one, 0)

    grad_some(0, nz)
    pl.when(core == 0)(lambda: give_grad())
    z_until(3, 3)
    if hi > 1:
        ring_step(1, 1)
    hidden_landing(1).wait_recv()
    down1 = functools.partial(down_block, 1)
    down_block(1, z)
    for d in range(1, lo + 1):
        use_near(3, d, down1)
    z_until(3, hi)
    use_far(3, down1)
    if hi > 2:
        ring_step(1, 2)

    def grad_step(d):
        if d == 0:
            grad_block(z, first=True)
        elif d <= lo:

            def both(i, carry):
                grad_block(plane_at(d - 2 * d * i))
                return carry

            lax.fori_loop(0, 2, both, 0)
        else:
            grad_block(plane_at(d))

    ring_done = [2 if hi > 2 else 1 if hi > 1 else 0]

    def ring_and_grad(first, last):
        @pl.when(core == 1)
        def _():
            for d in range(first, last):
                if d > ring_done[0]:
                    ring_step(1, d)
                grad_step(d)

    ring_and_grad(0, hi)
    finish_down(1)

    @pl.when(core == 1)
    def _():
        if hi > ring_done[0]:
            ring_step(1, hi)
        grad_block(plane_at(hi), parts=(0,))
        give_grad()
        grad_block(plane_at(hi), parts=(1,))


    await_bytes(st_rs.at[0], bytes_of(3, h2, feat))
    grad_copy().wait_recv()
    grad_copy().wait_send()

    block_bytes = bytes_of(feat, hidden)
    passed = 2 * sections * (2 * lo + 1) * block_bytes // 2
    await_bytes(hops, passed)
    await_bytes(pushes, passed + 2 * block_bytes)
    await_gains(gain_sends)
    await_bytes(
        others,
        bytes_of(2 * nt - 1, h2, feat)
        + bytes_of(nz - 1, part_rows, slice_width)
        + bytes_of(nt - 1, nz * part_rows, slice_width)
        + sections * bytes_of(h2, LANES, size=4)
        + (2 * sections + 1 + 2 * (nz - 1)) * bytes_of(h2, hidden)
        + (sections + 1) * bytes_of(nt - 1, rows, feat)
        + 3 * bytes_of(h2, feat),
    )


def stack(sizes, tokens, gain, w_up, w_down, cotangent):
    sections, dp_count, nt = sizes
    nz = dp_count // INNER
    assert sections == 2 and nz == nt and nz % 2 == 0
    rows, slice_width = tokens.shape
    feat = slice_width // INNER
    h2 = rows // sections
    hidden = w_up.shape[2]
    assert w_up.shape[1] == feat and w_down.shape[2] == feat
    width = slice_width * nt
    hi = nz // 2
    dma = pltpu.SemaphoreType.DMA
    hbm = pl.BlockSpec(memory_space=pl.ANY)
    vmem = pl.BlockSpec(memory_space=pltpu.VMEM)

    def buf(*dims, dtype=BF16):
        return pltpu.VMEM(dims, dtype)

    return pl.pallas_call(
        functools.partial(stack_kernel, sizes, width),
        name="stack",
        out_shape=(
            jax.ShapeDtypeStruct((rows, slice_width), BF16),
            jax.ShapeDtypeStruct((hidden, feat), F32),
            jax.ShapeDtypeStruct((hidden, feat), BF16),
        ),
        in_specs=[hbm] * 5,
        out_specs=(vmem, vmem, vmem),
        scratch_shapes=[
            buf(rows, slice_width),
            buf(1, slice_width),
            buf(1, slice_width, dtype=F32),
            buf(sections * nt, 1, feat, dtype=F32),
            buf(sections, nz, feat, hidden),
            buf(sections * nz * hidden, feat),
            buf(sections + 1, nt, rows, feat),
            buf(nt, rows, feat),
            buf(rows, LANES, dtype=F32),
            buf(rows, hidden, dtype=F32),
            buf(sections, h2, LANES, dtype=F32),
            buf(sections, h2, LANES, dtype=F32),
            buf(sections, h2, hidden),
            buf(sections, h2, hidden),
            buf(sections, rows, hidden),
            buf(sections, nt, rows, feat),
            buf(sections, nt, rows, feat),
            buf(nz, rows, hidden),
            buf(nz, rows, slice_width),
            buf(hidden, feat, dtype=F32),
            buf(hidden, feat),
            dma((5,)),
            dma((2,)),
            dma((1,)),
            dma((1,)),
            dma((3, PIECES, hi)),
            dma((2 * sections, hi + 1)),
            dma((1,)),
            dma((1,)),
            dma((sections,)),
            dma((sections,)),
            dma((sections,)),
            dma((sections,)),
            dma((2 * RING_PARTS, 2, hi)),
            dma((sections,)),
            dma((1,)),
            dma((1,)),
            dma((1,)),
        ],
        compiler_params=pltpu.CompilerParams(
            collective_id=0, has_side_effects=True, vmem_limit_bytes=VMEM_BYTES
        ),
    )(tokens, gain, w_up, w_down, cotangent)


def finish_kernel(state_ref, near_ref, far_ref, state_out, grad_out):
    state_out[0] = state_ref[...]
    grad_out[0] = (near_ref[...] + far_ref[...].astype(F32)).astype(BF16)


def finish(state, near, far):
    vmem = pl.BlockSpec(memory_space=pltpu.VMEM)
    return pl.pallas_call(
        finish_kernel,
        name="finish",
        out_shape=(
            jax.ShapeDtypeStruct((1, *state.shape), BF16),
            jax.ShapeDtypeStruct((1, *far.shape), BF16),
        ),
        in_specs=[vmem] * 3,
        out_specs=(vmem, vmem),
        compiler_params=pltpu.CompilerParams(vmem_limit_bytes=VMEM_BYTES // 4),
    )(state, near, far)


def body(tokens, gain, w_up, w_down, cotangent):
    sizes = (lax.axis_size("section"), lax.axis_size("dp"), lax.axis_size("tensor"))
    arrays = [
        pltpu.with_memory_space_constraint(array, pltpu.HBM)
        for array in (tokens, gain, w_up, w_down, cotangent)
    ]
    return finish(*stack(sizes, *arrays))


def solution(mesh):
    placed = (
        P("dp", "tensor"),
        P("section", "tensor"),
        P("section", "dp", "tensor"),
        P("section", "tensor", "dp"),
        P("section", "dp", None),
    )
    return jax.shard_map(
        body,
        mesh=mesh,
        in_specs=placed,
        out_specs=(P("section", "dp", "tensor"), P("section", "tensor", "dp")),
        check_vma=False,
    )
```

```python
import functools
import itertools

import jax
import jax.numpy as jnp
from jax import lax
from jax.experimental import pallas as pl
from jax.experimental.pallas import tpu as pltpu
from jax.sharding import PartitionSpec as P

EPS = 1e-06
F32 = jnp.float32
BF16 = jnp.bfloat16

MESH = pl.DeviceIdType.MESH
LANES = 128
PIECES = 4
INNER = 2
RING_PARTS = 2
VMEM_BYTES = 40 * 1024 * 1024


def far_first(count):
    return sorted(range(1, count), key=lambda k: abs(2 * k - count))


def remote(src, dst, send_sem, recv_sem, target):
    return pltpu.make_async_remote_copy(
        src_ref=src,
        dst_ref=dst,
        send_sem=send_sem,
        recv_sem=recv_sem,
        device_id=target,
        device_id_type=MESH,
    )


def stack_kernel(
    sizes,
    width,
    tok_ref,
    gain_ref,
    up_ref,
    down_ref,
    cot_ref,
    state_buf,
    near_out,
    grecv,
    tok,
    gain_raw,
    gain_f,
    gains,
    wu,
    wd,
    xb,
    xg,
    ssq,
    acc,
    sq_send,
    sq_recv,
    up_send,
    up_recv,
    hid,
    part_send,
    part_recv,
    hg,
    cb,
    gacc,
    gsend,
    send_sem,
    load_sem,
    tk_rs,
    ga_rs,
    z_rs,
    f_rs,
    c_rs,
    cs_rs,
    sq_rs,
    ux_rs,
    ax_rs,
    hd_rs,
    h_rs,
    p_rs,
    x_rs,
    st_rs,
    gx_rs,
):
    sections, dp_count, nt = sizes
    nz = dp_count // INNER
    hi = nz // 2
    lo = nz - 1 - hi
    rows, slice_width = tok.shape
    h2 = rows // sections
    feat = slice_width // INNER
    part_rows = rows // nt
    hidden = wu.shape[3]

    core = lax.axis_index("section")
    t = lax.axis_index("tensor")
    me = lax.axis_index("dp")
    z = me // INNER
    q = lax.rem(me, INNER)
    other = 1 - core
    sign = 1 - 2 * core
    beside = z * INNER + 1 - q

    def block_of(index, size):
        if isinstance(index, int):
            return pl.ds(index * size, size)
        return pl.ds(pl.multiple_of(index * size, size), size)

    mine = block_of(q, h2)
    theirs = block_of(1 - q, h2)
    core_rows = block_of(core, h2)
    other_rows = block_of(other, h2)
    my_cols = block_of(q, feat)
    their_cols = block_of(1 - q, feat)
    my_part = block_of(t, part_rows)

    hops, pushes, others, gain_sends, grad_sends = (send_sem.at[i] for i in range(5))

    def bytes_of(*dims, size=2):
        count = size
        for dim in dims:
            count *= dim
        return count

    def await_bytes(sem, count):
        ref = wd.at[pl.ds(0, count // (2 * feat))]
        pltpu.make_async_copy(ref, ref, sem).wait()

    def down_rows(layer, origin, piece=0, pieces=1):
        return block_of((layer * nz + origin) * pieces + piece, hidden // pieces)

    def tensor_at(off):
        return lax.rem(t + off, nt)

    def plane_at(shift):
        return lax.rem(z + nz + shift, nz)

    def launch(make, *args, cond=None):
        if cond is None:
            make(*args).start()
        else:
            pl.when(cond())(lambda: make(*args).start())

    loads = [
        pltpu.make_async_copy(up_ref.at[0], wu.at[core, z], load_sem.at[0]),
        pltpu.make_async_copy(tok_ref, tok, load_sem.at[0]),
        pltpu.make_async_copy(down_ref.at[0], wd.at[down_rows(core, z)], load_sem.at[0]),
        pltpu.make_async_copy(
            cot_ref.at[0, my_part, block_of(z, slice_width)], cb.at[z, my_part], load_sem.at[0]
        ),
    ]
    gain_load = pltpu.make_async_copy(gain_ref, gain_raw, load_sem.at[1])
    gain_load.start()
    for copy in loads:
        copy.start()

    barrier = pltpu.get_barrier_semaphore()

    def greet(target):
        pl.semaphore_signal(barrier, inc=1, device_id=target, device_id_type=MESH)

    for m in far_first(nz):
        greet({"dp": plane_at(m) * INNER + q})
    for off in far_first(nt) + [0]:
        greet({"dp": beside, "tensor": tensor_at(off)})
        greet({"section": other, "tensor": tensor_at(off)})
        if off:
            greet({"tensor": tensor_at(off)})
    greet({"section": other, "dp": beside})

    gain_load.wait()
    gain_f[...] = gain_raw[...].astype(F32)
    gains[core * nt + t] = gain_f[:, my_cols]
    ssq[...] = jnp.zeros_like(ssq)
    await_bytes(
        load_sem.at[0],
        bytes_of(2, feat, hidden) + bytes_of(rows, slice_width) + bytes_of(part_rows, slice_width),
    )
    xb[0, t, mine] = tok[core_rows, my_cols]

    pl.semaphore_wait(barrier, (nz - 1) + (2 * nt - 1) + nt + 1)

    def weight(layer, kind, origin, piece, pieces=PIECES):
        if kind:
            return wd.at[down_rows(layer, origin, piece, pieces)]
        return wu.at[layer, origin, block_of(piece, feat // pieces)]

    def along(d):
        return plane_at(-sign * d)

    def against(d):
        return plane_at(sign * d)

    def hop(m, piece, s):
        ref = weight(m // 2, m % 2, along(s), piece)
        return remote(
            ref,
            ref,
            hops,
            z_rs.at[m % 3, piece, s],
            {"dp": plane_at(sign) * INNER + q},
        )

    def landing(m, piece, d):
        ref = weight(m // 2, m % 2, along(d), piece)
        return remote(
            ref,
            ref,
            hops,
            z_rs.at[m % 3, piece, d - 1],
            {"dp": plane_at(sign) * INNER + q},
        )

    def push(m, piece, d):
        ref = weight(m // 2, m % 2, along(d), piece)
        return remote(
            ref, ref, pushes, f_rs.at[m, d], {"section": other}
        )

    def pushed(m, d):
        ref = weight(m // 2, m % 2, against(d), 0, 2 if d == hi else 1)
        return remote(ref, ref, pushes, f_rs.at[m, d], {"section": other})

    def push_own(kind, piece):
        ref = weight(core, kind, z, piece)
        m = 2 * core + kind
        return remote(
            ref, ref, pushes, f_rs.at[m, 0], {"section": other}
        )

    def lacks(layer):
        return lambda: core != layer

    half = PIECES // 2
    far_pieces = [core * half + j for j in range(half)]
    near_pieces = [other * half + j for j in range(half)]

    def begin(m):
        @pl.when(core != m // 2)
        def _():
            pushed(m, 0).wait_recv()

        for piece in range(PIECES) if lo else far_pieces:
            launch(hop, m, piece, 0)

    def advance(m, d, between=None):
        far = d >= lo
        for count, piece in enumerate(far_pieces if far else range(PIECES)):
            landing(m, piece, d).wait_recv()
            if d < hi:
                launch(hop, m, piece, d)
            launch(push, m, piece, d)
            if between is not None:
                between(count)
        if d == max(lo, 1) and m + 1 < 2 * sections:
            begin(m + 1)
        if d == lo:
            for count, piece in enumerate(near_pieces):
                landing(m, piece, d).wait_recv()
                launch(push, m, piece, d)
                if between is not None:
                    between(half + count)
        elif far and between is not None:
            for count in range(half, PIECES):
                between(count)

    rounds = [(m, d) for m in range(2 * sections) for d in range(1, hi + 1)]
    done_rounds = [0]

    def z_until(m, d, between=None):
        last = rounds.index((m, min(d, hi))) + 1
        for r in range(done_rounds[0], last):
            advance(*rounds[r], between if r == last - 1 else None)
        done_rounds[0] = max(done_rounds[0], last)

    def spread(count, do):
        def between(step):
            for i in range(step * count // PIECES, (step + 1) * count // PIECES):
                do(i)

        return between

    def take(m, d):
        pushed(m, d).wait_recv()

    def take_far(m):
        pushed(m, hi).wait_recv()

    for piece in range(PIECES):
        launch(push_own, 0, piece)

    @pl.when(core == 0)
    def _():
        for piece in range(PIECES) if lo else far_pieces:
            hop(0, piece, 0).start()

    def token_copy(away, off):
        cols, dp = (their_cols, beside) if away else (my_cols, me)
        return remote(
            tok.at[core_rows, cols],
            xb.at[0, t, mine],
            others,
            tk_rs.at[0],
            {"dp": dp, "tensor": tensor_at(off)},
        )

    for off in far_first(nt) + [0]:
        launch(token_copy, 1, off)
        if off:
            launch(token_copy, 0, off)

    def gain_copy(away, off):
        return remote(
            gains.at[core * nt + t],
            gains.at[core * nt + t],
            gain_sends,
            ga_rs.at[0],
            {"section": other if away else core, "tensor": tensor_at(off)},
        )

    def await_gains(sem):
        ref = gains.at[pl.ds(0, sections * nt - 1)]
        pltpu.make_async_copy(ref, ref, sem).wait()

    for off in far_first(nt) + [0]:
        launch(gain_copy, 1, off)
        if off:
            launch(gain_copy, 0, off)
    for piece in range(PIECES):
        launch(push_own, 1, piece)

    def cot_copy(m):
        to = plane_at(m)
        return remote(
            cot_ref.at[0, my_part, block_of(to, slice_width)],
            cb.at[z, my_part],
            others,
            c_rs.at[0],
            {"dp": to * INNER + q},
        )

    for m in far_first(nz):
        launch(cot_copy, m)

    @pl.when(core != 0)
    def _():
        pushed(0, 0).wait_recv()
        for piece in range(PIECES) if lo else far_pieces:
            hop(0, piece, 0).start()


    def cot_share(off):
        ref = cb.at[:, my_part]
        return remote(ref, ref, others, cs_rs.at[0], {"tensor": tensor_at(off)})

    def await_cotangent():
        await_bytes(c_rs.at[0], bytes_of(nz - 1, part_rows, slice_width))

    def share_cotangent(first, last):
        for off in far_first(nt)[first:last]:
            launch(cot_share, off)

    def prepare(layer, block):
        x = xb[layer, block].astype(F32)
        xg[block] = (x * gains[layer * nt + block]).astype(BF16)
        square = x * x
        total = ssq[...]
        for lower in range(0, feat, LANES):
            total = total + square[:, lower : lower + LANES]
        ssq[...] = total

    def up_block(layer, block, first=False):
        value = jnp.dot(xg[block], wu[layer, block], preferred_element_type=F32)
        acc[...] = value if first else acc[...] + value

    def sum_copy(layer):
        return remote(
            sq_send.at[layer], sq_recv.at[layer], others, sq_rs.at[layer], {"dp": beside}
        )

    def send_sums(layer):
        sq_send[layer] = jnp.broadcast_to(
            jnp.sum(ssq[theirs], axis=1, keepdims=True), (h2, LANES)
        )
        launch(sum_copy, layer)

    def up_copy(layer):
        return remote(
            up_send.at[layer], up_recv.at[layer], others, ux_rs.at[layer], {"dp": beside}
        )

    def send_up(layer):
        up_send[layer] = acc[theirs].astype(BF16)
        launch(up_copy, layer)

    def hidden_copy(layer):
        ref = hid.at[layer, mine]
        return remote(ref, ref, others, ax_rs.at[layer], {"dp": beside})

    def hidden_landing(layer):
        ref = hid.at[layer, theirs]
        return remote(ref, ref, others, ax_rs.at[layer], {"dp": beside})

    def hidden_give(layer):
        return remote(
            hid.at[layer, mine],
            hg.at[z, core_rows],
            others,
            hd_rs.at[layer],
            {"section": other},
        )

    def hidden_given(layer):
        ref = hg.at[z, other_rows]
        return remote(ref, ref, others, hd_rs.at[layer], {"section": other})

    def finish_up(layer):
        sum_copy(layer).wait_recv()
        total = jnp.sum(ssq[mine], axis=1, keepdims=True) + sq_recv[layer]
        inverse = lax.rsqrt(total / width + EPS)
        up_copy(layer).wait_recv()
        for lower in range(0, hidden, LANES):
            cols = pl.ds(lower, LANES)
            value = (acc[mine, cols] + up_recv[layer, :, cols].astype(F32)) * inverse
            hid[layer, mine, cols] = jax.nn.gelu(value, approximate=True).astype(BF16)
        launch(hidden_copy, layer)
        launch(hidden_give, layer, cond=lacks(layer))

        @pl.when(core == layer)
        def _():
            hg[z, core_rows] = hid[layer, mine]

        if layer == 0:
            ssq[...] = jnp.zeros_like(ssq)

    def ring_length(k, way):
        return hi if k == way else lo

    def ring_ref(k, part, origin, layer):
        whose = layer if k == 0 else 1 - layer
        return hg.at[origin, block_of(whose * RING_PARTS + part, h2 // RING_PARTS)]

    def ring_copy(k, part, way, s, layer):
        delta = 1 if way == 0 else -1
        ref = ring_ref(k, part, plane_at(-delta * s), layer)
        return remote(
            ref,
            ref,
            others,
            h_rs.at[k * RING_PARTS + part, way, s],
            {"dp": plane_at(delta) * INNER + q},
        )

    def ring_landing(k, part, way, d, layer):
        delta = 1 if way == 0 else -1
        ref = ring_ref(k, part, plane_at(-delta * d), layer)
        return remote(
            ref,
            ref,
            others,
            h_rs.at[k * RING_PARTS + part, way, d - 1],
            {"dp": plane_at(delta) * INNER + q},
        )

    def ring_step(layer, d):
        @pl.when(core == layer)
        def _():
            for k in range(2):
                if d == 0 and k == 1:
                    hidden_given(layer).wait_recv()
                for part, way in itertools.product(range(RING_PARTS), range(2)):
                    length = ring_length(k, way)
                    if 0 < d <= length:
                        ring_landing(k, part, way, d, layer).wait_recv()
                    if d < length:
                        ring_copy(k, part, way, d, layer).start()

    def part_copy(layer, block):
        return remote(
            part_send.at[layer, block],
            part_recv.at[layer, t],
            others,
            p_rs.at[layer],
            {"tensor": block},
        )

    def down_block(layer, block):
        part_send[layer, block] = jnp.dot(
            hid[layer], wd[down_rows(layer, block)], preferred_element_type=F32
        ).astype(BF16)

        @pl.when(block != t)
        def _():
            part_copy(layer, block).start()

    def next_copy(off):
        ref = xb.at[1, t]
        return remote(ref, ref, others, x_rs.at[0], {"tensor": tensor_at(off)})

    def state_copy(layer, away):
        return remote(
            xb.at[layer + 1, t, theirs if away else mine],
            state_buf.at[core_rows, my_cols],
            others,
            st_rs.at[0],
            {"section": layer, "dp": beside} if away else {"section": other},
        )

    def finish_down(layer):
        value = xb[layer, t].astype(F32) + part_send[layer, t].astype(F32)
        await_bytes(p_rs.at[layer], bytes_of(nt - 1, rows, feat))
        for off in range(1, nt):
            value = value + part_recv[layer, tensor_at(off)].astype(F32)
        xb[layer + 1, t] = value.astype(BF16)
        if layer == 0:
            for off in far_first(nt):
                launch(next_copy, off)
        launch(state_copy, layer, 1)
        launch(state_copy, layer, 0, cond=lacks(layer))

        @pl.when(core == layer)
        def _():
            state_buf[core_rows, my_cols] = xb[layer + 1, t, mine]

    def grad_block(origin, first=False, parts=(0, 1)):
        left = hg[origin]
        for index in parts:
            cols = my_cols if index else their_cols
            value = lax.dot_general(
                left, cb[origin, :, cols], (((0,), (0,)), ((), ())), preferred_element_type=F32
            )
            total = near_out if index else gacc
            total[...] = value if first else total[...] + value

    def grad_copy():
        return remote(gsend, grecv, grad_sends, gx_rs.at[0], {"dp": beside})

    def give_grad():
        gsend[...] = gacc[...].astype(BF16)
        grad_copy().start()

    z_until(0, 2)
    await_bytes(tk_rs.at[0], bytes_of(2 * nt - 1, h2, feat))
    await_gains(ga_rs.at[0])

    def prepare_first(block, carry):
        prepare(0, block)
        return carry

    lax.fori_loop(0, nt, prepare_first, 0)
    send_sums(0)

    def use_near(m, d, use):
        use(along(d))
        take(m, d)
        use(against(d))

    def use_far(m, use):
        take_far(m)
        use(along(hi))

    up0 = functools.partial(up_block, 0)
    up_block(0, z, first=True)
    for d in range(1, lo + 1):
        z_until(0, d + 1)
        use_near(0, d, up0)
    z_until(0, hi)
    use_far(0, up0)
    send_up(0)
    await_cotangent()
    z_until(1, 1)
    finish_up(0)
    share_cotangent(0, nt // 2 - 1)
    z_until(1, hi)
    ring_step(0, 0)
    down0 = functools.partial(down_block, 0)
    hidden_landing(0).wait_recv()
    down_block(0, z)
    for d in range(1, lo + 1):
        use_near(1, d, down0)
    use_far(1, down0)
    z_until(2, 1)
    if hi > 1:
        ring_step(0, 1)
    z_until(2, 2)
    finish_down(0)
    share_cotangent(nt // 2 - 1, nt)
    if hi > 2:
        ring_step(0, 2)
    z_until(2, hi)

    for d in range(1, lo + 1):
        take(2, d)
    take_far(2)
    await_bytes(x_rs.at[0], bytes_of(nt - 1, rows, feat))

    def up_second(off):
        prepare(1, tensor_at(off))
        up_block(1, tensor_at(off), first=off == 0)

    z_until(3, 1, spread(nt, up_second))
    send_sums(1)
    send_up(1)
    if hi > 3:
        ring_step(0, 3)
    z_until(3, 2)
    finish_up(1)
    ring_step(1, 0)
    ring_step(0, hi)
    await_bytes(cs_rs.at[0], bytes_of(nt - 1, nz * part_rows, slice_width))

    def grad_some(first, last):
        @pl.when(core == 0)
        def _():
            if first == 0:
                grad_block(z, first=True)

            def one(i, carry):
                grad_block(plane_at(i))
                return carry

            lax.fori_loop(max(first, 1), last, one, 0)

    grad_some(0, nz)
    pl.when(core == 0)(lambda: give_grad())
    z_until(3, 3)
    if hi > 1:
        ring_step(1, 1)
    z_until(3, hi)
    hidden_landing(1).wait_recv()
    down1 = functools.partial(down_block, 1)
    down_block(1, z)
    for d in range(1, lo + 1):
        if d == lo and hi > 2:
            ring_step(1, 2)
        use_near(3, d, down1)
    use_far(3, down1)

    def grad_step(d):
        if d == 0:
            grad_block(z, first=True)
        elif d <= lo:

            def both(i, carry):
                grad_block(plane_at(d - 2 * d * i))
                return carry

            lax.fori_loop(0, 2, both, 0)
        else:
            grad_block(plane_at(d))

    ring_done = [2 if hi > 2 else 1 if hi > 1 else 0]

    def ring_and_grad(first, last):
        @pl.when(core == 1)
        def _():
            for d in range(first, last):
                if d > ring_done[0]:
                    ring_step(1, d)
                grad_step(d)

    ring_and_grad(0, hi)
    finish_down(1)

    @pl.when(core == 1)
    def _():
        if hi > ring_done[0]:
            ring_step(1, hi)
        grad_block(plane_at(hi), parts=(0,))
        give_grad()
        grad_block(plane_at(hi), parts=(1,))


    await_bytes(st_rs.at[0], bytes_of(3, h2, feat))
    grad_copy().wait_recv()
    grad_copy().wait_send()

    block_bytes = bytes_of(feat, hidden)
    passed = 2 * sections * (2 * lo + 1) * block_bytes // 2
    await_bytes(hops, passed)
    await_bytes(pushes, passed + 2 * block_bytes)
    await_gains(gain_sends)
    await_bytes(
        others,
        bytes_of(2 * nt - 1, h2, feat)
        + bytes_of(nz - 1, part_rows, slice_width)
        + bytes_of(nt - 1, nz * part_rows, slice_width)
        + sections * bytes_of(h2, LANES, size=4)
        + (2 * sections + 1 + 2 * (nz - 1)) * bytes_of(h2, hidden)
        + (sections + 1) * bytes_of(nt - 1, rows, feat)
        + 3 * bytes_of(h2, feat),
    )


def stack(sizes, tokens, gain, w_up, w_down, cotangent):
    sections, dp_count, nt = sizes
    nz = dp_count // INNER
    assert sections == 2 and nz == nt and nz % 2 == 0
    rows, slice_width = tokens.shape
    feat = slice_width // INNER
    h2 = rows // sections
    hidden = w_up.shape[2]
    assert w_up.shape[1] == feat and w_down.shape[2] == feat
    width = slice_width * nt
    hi = nz // 2
    dma = pltpu.SemaphoreType.DMA
    hbm = pl.BlockSpec(memory_space=pl.ANY)
    vmem = pl.BlockSpec(memory_space=pltpu.VMEM)

    def buf(*dims, dtype=BF16):
        return pltpu.VMEM(dims, dtype)

    return pl.pallas_call(
        functools.partial(stack_kernel, sizes, width),
        name="stack",
        out_shape=(
            jax.ShapeDtypeStruct((rows, slice_width), BF16),
            jax.ShapeDtypeStruct((hidden, feat), F32),
            jax.ShapeDtypeStruct((hidden, feat), BF16),
        ),
        in_specs=[hbm] * 5,
        out_specs=(vmem, vmem, vmem),
        scratch_shapes=[
            buf(rows, slice_width),
            buf(1, slice_width),
            buf(1, slice_width, dtype=F32),
            buf(sections * nt, 1, feat, dtype=F32),
            buf(sections, nz, feat, hidden),
            buf(sections * nz * hidden, feat),
            buf(sections + 1, nt, rows, feat),
            buf(nt, rows, feat),
            buf(rows, LANES, dtype=F32),
            buf(rows, hidden, dtype=F32),
            buf(sections, h2, LANES, dtype=F32),
            buf(sections, h2, LANES, dtype=F32),
            buf(sections, h2, hidden),
            buf(sections, h2, hidden),
            buf(sections, rows, hidden),
            buf(sections, nt, rows, feat),
            buf(sections, nt, rows, feat),
            buf(nz, rows, hidden),
            buf(nz, rows, slice_width),
            buf(hidden, feat, dtype=F32),
            buf(hidden, feat),
            dma((5,)),
            dma((2,)),
            dma((1,)),
            dma((1,)),
            dma((3, PIECES, hi)),
            dma((2 * sections, hi + 1)),
            dma((1,)),
            dma((1,)),
            dma((sections,)),
            dma((sections,)),
            dma((sections,)),
            dma((sections,)),
            dma((2 * RING_PARTS, 2, hi)),
            dma((sections,)),
            dma((1,)),
            dma((1,)),
            dma((1,)),
        ],
        compiler_params=pltpu.CompilerParams(
            collective_id=0, has_side_effects=True, vmem_limit_bytes=VMEM_BYTES
        ),
    )(tokens, gain, w_up, w_down, cotangent)


def finish_kernel(state_ref, near_ref, far_ref, state_out, grad_out):
    state_out[0] = state_ref[...]
    grad_out[0] = (near_ref[...] + far_ref[...].astype(F32)).astype(BF16)


def finish(state, near, far):
    vmem = pl.BlockSpec(memory_space=pltpu.VMEM)
    return pl.pallas_call(
        finish_kernel,
        name="finish",
        out_shape=(
            jax.ShapeDtypeStruct((1, *state.shape), BF16),
            jax.ShapeDtypeStruct((1, *far.shape), BF16),
        ),
        in_specs=[vmem] * 3,
        out_specs=(vmem, vmem),
        compiler_params=pltpu.CompilerParams(vmem_limit_bytes=VMEM_BYTES // 4),
    )(state, near, far)


def body(tokens, gain, w_up, w_down, cotangent):
    sizes = (lax.axis_size("section"), lax.axis_size("dp"), lax.axis_size("tensor"))
    arrays = [
        pltpu.with_memory_space_constraint(array, pltpu.HBM)
        for array in (tokens, gain, w_up, w_down, cotangent)
    ]
    return finish(*stack(sizes, *arrays))


def solution(mesh):
    placed = (
        P("dp", "tensor"),
        P("section", "tensor"),
        P("section", "dp", "tensor"),
        P("section", "tensor", "dp"),
        P("section", "dp", None),
    )
    return jax.shard_map(
        body,
        mesh=mesh,
        in_specs=placed,
        out_specs=(P("section", "dp", "tensor"), P("section", "tensor", "dp")),
        check_vma=False,
    )
```
